256 devices in a mesh: grp: 2 (over y), seq: 128 (over x, z, core).
Axes of the slice: x: 4, y: 2, z: 16, core: 2. Of those that a mesh axis runs over, the one named last changes fastest.
The devices are a block of a 4x16x16 slice.
Arguments:
- queries: bfloat16 [32768, 12288], P(('grp', 'seq')), parts along dimension 0, may hold values from -8 to 8
- sum_keys: bfloat16 [2048, 768], P(('grp', 'seq')), parts along dimension 0, may hold values from -4 to 4
- sum_values: bfloat16 [2048, 512], P(('grp', 'seq')), parts along dimension 0, may hold values from -24 to 24
- limits: int32 [512], P('grp'), parts along dimension 0, may hold values from 1 to 1024, as said below
- valid_tokens: int32 [2], P('grp'), parts along dimension 0, may hold values from 8192 to 16384
Outputs:
- attended: bfloat16 [32768, 8192], P(('grp', 'seq')), parts along dimension 0
The draws below stay inside these ranges and needn't reach their ends.
There are 2 independent parts, one for each index of `grp`. The reference program is written for one: setup_inputs(seed, part) draws one part's arguments, and reference() takes and returns one part's arrays. A program takes and returns all parts, laid end to end along the dimension named above; each array names one. Nothing has to cross between parts.
Inputs may be any that keep to these rules, and one draw needn't show every extreme that they name: limits[b] is at least 1 and at most max(1, (64 * b - 32) // 16 + 1), the number of summaries that end at or before the block's first token; the last block reaches this bound.
All inputs are finite; a program needn't handle non-finite values.
Results may differ from the reference program's by a relative error of at most 0.0027.
Values may be sent and summed in bfloat16 or wider, within the bound.
A program may use at most 64 MiB of HBM per device.

```python
import jax
import jax.numpy as jnp
from jax import lax

H = 64
G = 4
DK = 192
DV = 128
STRIDE = 16
CBLOCK = 32
QB = 64
L = 16384
NS = 1024
NB = 256


def summary_key_law(key):
    inner = jax.random.fold_in(key, 11)
    values = jnp.clip(jax.random.normal(inner, (NS, G * DK)), -4.0, 4.0)
    return values.astype(jnp.float32)


def draw_sum_keys(key, part):
    return summary_key_law(key).astype(jnp.bfloat16)


def draw_queries(key, part):
    inner = jax.random.fold_in(key, 23)
    values = jnp.clip(2.5 * jax.random.normal(inner, (L, H * DK)), -8.0, 8.0)
    return values.astype(jnp.bfloat16)


def draw_limits(key, part):
    block_ids = jnp.arange(NB, dtype=jnp.int32)
    causal = jnp.maximum((QB * block_ids - CBLOCK) // STRIDE + 1, 1).astype(jnp.int32)
    offsets = jax.random.randint(jax.random.fold_in(key, 5), (NB,), 0, 1 << 20, dtype=jnp.int32) % (causal // 4 + 1)
    drawn = causal - offsets
    return drawn.at[NB - 1].set(causal[NB - 1]).astype(jnp.int32)


def shard_levels(stream_key, dims, pieces, smallest, high):
    def one(dim, parts):
        heights = jax.random.uniform(jax.random.fold_in(jax.random.fold_in(stream_key, 6), dim), (parts,), jnp.float32, smallest / len(pieces), high / len(pieces))
        return jnp.repeat(jnp.exp(heights), dims[dim] // parts).reshape((-1,) + (1,) * (len(dims) - dim - 1))

    loudness = one(*pieces[0])
    for cut in pieces[1:]:
        loudness = loudness * one(*cut)
    return loudness


def scatter_about(own_key, extent, scale, most, cuts=(), kind=jnp.bfloat16):
    gain = shard_levels(own_key, extent, cuts, -0.22, 0.18) if cuts else 1.0
    result = jax.random.normal(own_key, extent, jnp.float32) * scale * gain
    return jnp.minimum(jnp.maximum(result, -most), most).astype(kind)


def setup_inputs(seed: int = 0, part: int = 0) -> dict:
    splits = jax.random.split(jax.random.key(seed), 6)
    part_splits = jax.random.split(jax.random.fold_in(splits[5], part), 6)
    return {
        "queries": draw_queries(jax.random.fold_in(jax.random.fold_in(splits[5], part), 71), part),
        "sum_keys": draw_sum_keys(jax.random.fold_in(jax.random.fold_in(splits[5], part), 71), part),
        "sum_values": scatter_about(part_splits[2], (NS, G * DV), 4.0, 24.0, ((0, 128),)),
        "limits": draw_limits(jax.random.fold_in(jax.random.fold_in(splits[5], part), 71), part),
        "valid_tokens": jax.random.randint(part_splits[4], (1,), L // 2, L + 1).astype(jnp.int32),
    }


def reference(queries, sum_keys, sum_values, limits, valid_tokens):
    per_group = H // G
    inv_root = float(DK) ** -0.5
    usable = jnp.maximum((valid_tokens[0] - CBLOCK) // STRIDE + 1, 1).astype(jnp.int32)
    key_table = sum_keys.reshape(NS, G, DK).astype(jnp.float32)
    value_table = sum_values.reshape(NS, G, DV).astype(jnp.float32)
    summary_ids = jnp.arange(NS, dtype=jnp.int32)

    def one_block(block_args):
        query_block, block_limit = block_args
        grouped = query_block.reshape(QB, G, per_group, DK).astype(jnp.float32)
        scores = jnp.einsum("tgjd,sgd->tgjs", grouped, key_table, precision=lax.Precision.HIGHEST) * inv_root
        visible = summary_ids < jnp.minimum(block_limit, usable)
        scores = jnp.where(visible, scores, -1e30)
        row_max = jnp.max(scores, axis=-1, keepdims=True)
        weights = jnp.where(visible, jnp.exp(scores - row_max), 0.0)
        row_total = jnp.sum(weights, axis=-1, keepdims=True)
        rounded = lax.optimization_barrier(weights.astype(jnp.bfloat16)).astype(jnp.float32)
        blended = jnp.einsum("tgjs,sgd->tgjd", rounded, value_table, precision=lax.Precision.HIGHEST) / row_total
        return blended.reshape(QB, H * DV).astype(jnp.bfloat16)

    blocks = lax.map(one_block, (queries.reshape(NB, QB, H * DK), limits))
    return blocks.reshape(L, H * DV)
```

```python
import functools

import jax
import jax.numpy as jnp
from jax import lax
from jax.experimental import pallas as pl
from jax.experimental.pallas import tpu as pltpu
from jax.sharding import PartitionSpec as P

H = 64
G = 4
DK = 192
DV = 128
STRIDE = 16
CBLOCK = 32
QB = 64

CORES = 2
COLS = 4
ROUNDS = 4
PAD = 256
ROWS = 256
UNROLL = 4
NEG = -1e30
SCALE = float(DK) ** -0.5 * 1.4426950408889634


def steps_along_z(r):
    near, far = 2 * r + 1, 2 * r + 2
    return (-near, -far, near, far) if r < ROUNDS - 1 else (-near, -far, near, 0)


def slot_of(r, core, col, j):
    return ((r * CORES + core) * COLS + col) * 4 + j


def place(depth):
    me = lax.axis_index("seq")
    return me // (depth * CORES), lax.rem(me // CORES, depth), lax.rem(me, CORES)


def gather_kernel(depth, k_ref, v_ref, kv, own_sem, z_send, z_recv, x_send, x_recv, d_send, d_recv):
    col, z, core = place(depth)

    def device(dx, dz, dc):
        target = lax.rem(col + dx + COLS, COLS) * (depth * CORES) + lax.rem(z + dz + depth, depth) * CORES
        return {"seq": target + lax.rem(core + dc, CORES)}

    own = slot_of(ROUNDS - 1, core, col, 3)
    copies = [
        pltpu.make_async_copy(k_ref, kv.at[own, :, 0 : G * DK], own_sem.at[0]),
        pltpu.make_async_copy(v_ref, kv.at[own, :, G * DK : G * (DK + DV)], own_sem.at[1]),
    ]
    for c in copies:
        c.start()
    partners = [device(0, dz, 0) for dz in (1, 2, -1, -2)] + [device(dx, 0, 0) for dx in (1, 2, 3)] + [device(0, 0, 1)]
    barrier = pltpu.get_barrier_semaphore()
    for p in partners:
        pl.semaphore_signal(barrier, inc=1, device_id=p, device_id_type=pl.DeviceIdType.MESH)
    pl.semaphore_wait(barrier, len(partners))
    for c in copies:
        c.wait()

    sent = []

    def push(src, dst, send, recv, target):
        c = pltpu.make_async_remote_copy(
            src_ref=src, dst_ref=dst, send_sem=send, recv_sem=recv, device_id=target, device_id_type=pl.DeviceIdType.MESH
        )
        c.start()
        sent.append(c)

    def relay_z(r, up, down):
        order = ((1, up, 1), (3, down, -1), (0, up, 1), (2, down, -1))
        for j, src, way in order:
            if src is None or (r == ROUNDS - 1 and j == 3):
                continue
            far = 2 if j in (1, 3) else 1
            push(kv.at[src], kv.at[slot_of(r, core, col, j)], z_send.at[r * 4 + j], z_recv.at[r * 4 + j], device(0, way * far, 0))

    def across(s, r, slab):
        for dx in (2, 1, 3):
            push(slab, slab, x_send.at[s * 3 + dx - 1], x_recv.at[s * 3 + dx - 1], device(dx, 0, 0))

    def pair(s, k, slab):
        push(slab, slab, d_send.at[s * COLS + k], d_recv.at[s * COLS + k], device(0, 0, 1))

    def slab_of(s, column, of_core):
        if s == ROUNDS:
            return kv.at[pl.ds(slot_of(ROUNDS - 1, of_core, column, 3), 1)]
        return kv.at[pl.ds(slot_of(s, of_core, column, 0), 3 if s == ROUNDS - 1 else 4)]

    def arrived(slab, sem):
        pltpu.make_async_copy(slab, slab, sem).wait()

    def column(k):
        return lax.rem(col - k + COLS, COLS)

    def pass_on(s):
        for k in (1, 3, 2):
            slab = slab_of(s, column(k), core)
            arrived(slab, x_recv.at[s * 3 + k - 1])
            pair(s, k, slab)

    mine = slab_of(ROUNDS, col, core)
    relay_z(0, own, own)
    across(ROUNDS, ROUNDS - 1, mine)
    pair(ROUNDS, 0, mine)
    for r in range(ROUNDS):
        for j in range(4):
            if not (r == ROUNDS - 1 and j == 3):
                at = slot_of(r, core, col, j)
                arrived(kv.at[at], z_recv.at[r * 4 + j])
        if r < ROUNDS - 1:
            relay_z(r + 1, slot_of(r, core, col, 1), slot_of(r, core, col, 3))
        slab = slab_of(r, col, core)
        across(r, r, slab)
        pair(r, 0, slab)
        pass_on(ROUNDS if r == 0 else r - 1)
    pass_on(ROUNDS - 1)
    for s in range(ROUNDS + 1):
        for k in range(COLS):
            arrived(slab_of(s, column(k), 1 - core), d_recv.at[s * COLS + k])
    for c in sent:
        c.wait_send()


def spread_queries(q_ref, qp):
    tokens = q_ref.shape[0]
    lane = lax.broadcasted_iota(jnp.int32, (tokens, PAD), 1)
    token = lax.broadcasted_iota(jnp.int32, (tokens, PAD), 0)
    for head in range(H):
        group = head // (H // G)
        low = group % 2 == 0
        first = head * DK
        spare = DK if low else 0
        marks = jnp.where(lane == spare + token // QB, 1.0, 0.0)
        window = q_ref[:, pl.ds(first - first % 128, PAD)].astype(jnp.float32)
        if low != (first % 128 == 0):
            window = pltpu.roll(window, PAD - 64 if low else 64, 1)
        held = jnp.where((lane < DK) if low else (lane >= PAD - DK), window, marks)
        qp[head * tokens : (head + 1) * tokens, :] = held.astype(jnp.bfloat16)


def spread_keys(r, depth, caps, kv, kp, vp):
    col, z, core = place(depth)
    keys = CORES * COLS * 4 * 8
    block = kv[pl.ds(r * CORES * COLS * 4, CORES * COLS * 4)].astype(jnp.float32).reshape(keys, G * (DK + DV))
    at = lax.broadcasted_iota(jnp.int32, (keys, PAD), 0)
    lane = lax.broadcasted_iota(jnp.int32, (keys, PAD), 1)
    j = (at // 8) % 4
    steps = steps_along_z(r)
    shift = jnp.where(j == 0, steps[0], jnp.where(j == 1, steps[1], jnp.where(j == 2, steps[2], steps[3])))
    source_z = (z + shift + depth) % depth
    source = ((at // 32) % COLS) * (depth * CORES) + source_z * CORES + at // (32 * COLS)
    ids = source * 8 + at % 8
    for group in range(G):
        low = group % 2 == 0
        first = group * DK
        spare = DK if low else 0
        hidden = ((lane == spare) & (ids >= caps[0])) | ((lane == spare + 1) & (ids >= caps[1]))
        bias = jnp.where(hidden, NEG, 0.0)
        window = block[:, first - first % 128 : first - first % 128 + PAD]
        held = jnp.where((lane < DK) if low else (lane >= PAD - DK), window, bias)
        kp[group] = held.astype(jnp.bfloat16)
        vp[group] = block[:, G * DK + group * DV : G * DK + (group + 1) * DV].astype(jnp.bfloat16)


def fold(first, last, tokens, qp, kp, vp, top, total, held, out_ref):
    per_group = H // G * tokens

    def step(i, carry):
        for u in range(UNROLL):
            at = pl.multiple_of((i * UNROLL + u) * ROWS, ROWS)
            rows = pl.ds(at, ROWS)
            group = (i * UNROLL) * ROWS // per_group
            score = lax.dot_general(
                qp[rows, :], kp[group], (((1,), (1,)), ((), ())), preferred_element_type=jnp.float32
            )
            best = jnp.max(score, axis=1, keepdims=True) * SCALE
            if first:
                new_top = jnp.broadcast_to(best, (ROWS, 128))
            else:
                old_top = top[rows, :]
                new_top = jnp.maximum(old_top, best)
            parts = [jnp.exp2(score[:, c : c + 128] * SCALE - new_top) for c in range(0, score.shape[1], 128)]
            weight = jnp.concatenate(parts, axis=1)
            added = sum(parts[1:], parts[0])
            value = jnp.dot(weight.astype(jnp.bfloat16), vp[group], preferred_element_type=jnp.float32)
            if not first:
                rescale = jnp.exp2(old_top - new_top)
                added = added + total[rows, :] * rescale
                value = value + held[rows, :] * rescale
            if last:
                norm = jnp.sum(added, axis=1, keepdims=True)
                done = (value / norm).astype(jnp.bfloat16)
                for b in range(ROWS // tokens):
                    head = (i * UNROLL + u) * (ROWS // tokens) + b
                    out_ref[:, pl.ds(pl.multiple_of(head * DV, DV), DV)] = done[b * tokens : (b + 1) * tokens]
            else:
                top[rows, :] = new_top
                total[rows, :] = added
                held[rows, :] = value
        return carry

    lax.fori_loop(0, H * tokens // (ROWS * UNROLL), step, 0)


def attend_kernel(depth, q_ref, kv, limits, valid, out_ref, qp, kp, vp, top, total, held):
    tokens = q_ref.shape[0]
    usable = jnp.maximum(lax.shift_right_arithmetic(valid[0] - CBLOCK, 4) + 1, 1)
    mine = lax.axis_index("seq") * (tokens // QB)
    caps = [jnp.minimum(limits[mine + b], usable) for b in range(tokens // QB)]
    spread_queries(q_ref, qp)
    for r in range(ROUNDS):
        spread_keys(r, depth, caps, kv, kp, vp)
        fold(r == 0, r == ROUNDS - 1, tokens, qp, kp, vp, top, total, held, out_ref)


def per_device(depth, queries, sum_keys, sum_values, limits, valid_tokens):
    tokens = queries.shape[0]
    width = G * (DK + DV)
    slots = ROUNDS * CORES * COLS * 4
    vmem = pl.BlockSpec(memory_space=pltpu.VMEM)
    smem = pl.BlockSpec(memory_space=pltpu.SMEM)
    anywhere = pl.BlockSpec(memory_space=pl.ANY)
    dma = pltpu.SemaphoreType.DMA
    kv = pl.pallas_call(
        functools.partial(gather_kernel, depth),
        out_shape=jax.ShapeDtypeStruct((slots, sum_keys.shape[0], width), jnp.bfloat16),
        in_specs=[anywhere, anywhere],
        out_specs=vmem,
        scratch_shapes=[
            dma((2,)),
            dma((ROUNDS * 4,)),
            dma((ROUNDS * 4,)),
            dma((ROUNDS * 3 + 3,)),
            dma((ROUNDS * 3 + 3,)),
            dma((ROUNDS * COLS + COLS,)),
            dma((ROUNDS * COLS + COLS,)),
        ],
        compiler_params=pltpu.CompilerParams(collective_id=0, has_side_effects=True),
        name="gather",
    )(sum_keys, sum_values)
    keys = CORES * COLS * 4 * sum_keys.shape[0]
    rows = H * tokens
    return pl.pallas_call(
        functools.partial(attend_kernel, depth),
        out_shape=jax.ShapeDtypeStruct((tokens, H * DV), jnp.bfloat16),
        in_specs=[vmem, vmem, smem, smem],
        out_specs=vmem,
        scratch_shapes=[
            pltpu.VMEM((rows, PAD), jnp.bfloat16),
            pltpu.VMEM((G, keys, PAD), jnp.bfloat16),
            pltpu.VMEM((G, keys, DV), jnp.bfloat16),
            pltpu.VMEM((rows, 128), jnp.float32),
            pltpu.VMEM((rows, 128), jnp.float32),
            pltpu.VMEM((rows, DV), jnp.float32),
        ],
        name="attend",
    )(queries, kv, limits, valid_tokens)


def solution(mesh):
    depth = mesh.shape["seq"] // (COLS * CORES)
    placed = (
        P(("grp", "seq"), None),
        P(("grp", "seq"), None),
        P(("grp", "seq"), None),
        P("grp"),
        P("grp"),
    )
    return jax.shard_map(
        functools.partial(per_device, depth),
        mesh=mesh,
        in_specs=placed,
        out_specs=P(("grp", "seq"), None),
        check_vma=False,
    )
```

```python
import functools

import jax
import jax.numpy as jnp
from jax import lax
from jax.experimental import pallas as pl
from jax.experimental.pallas import tpu as pltpu
from jax.sharding import PartitionSpec as P

H = 64
G = 4
DK = 192
DV = 128
STRIDE = 16
CBLOCK = 32
QB = 64

CORES = 2
COLS = 4
ROUNDS = 4
UP, DOWN = 0, 1
PAD = 256
ROWS = 256
AHEAD = 3
NEG = -1e30
SCALE = float(DK) ** -0.5 * 1.4426950408889634


def place(depth):
    me = lax.axis_index("seq")
    return me // (depth * CORES), lax.rem(me // CORES, depth), lax.rem(me, CORES)


def spread_queries(q_ref, qp):
    tokens = q_ref.shape[0]
    lane = lax.broadcasted_iota(jnp.int32, (tokens, PAD), 1)
    token = lax.broadcasted_iota(jnp.int32, (tokens, PAD), 0)
    for head in range(H):
        group = head // (H // G)
        low = group % 2 == 0
        first = head * DK
        spare = DK if low else 0
        marks = jnp.where(lane == spare + token // QB, 1.0, 0.0)
        window = q_ref[:, pl.ds(first - first % 128, PAD)].astype(jnp.float32)
        if low != (first % 128 == 0):
            window = pltpu.roll(window, PAD - 64 if low else 64, 1)
        held = jnp.where((lane < DK) if low else (lane >= PAD - DK), window, marks)
        qp[head * tokens : (head + 1) * tokens, :] = held.astype(jnp.bfloat16)


def spread_keys(part, depth, caps, kv, kp, vp):
    col, z, core = place(depth)
    keys = CORES * COLS * 4 * 8
    slots = keys // 8
    block = kv[pl.ds(part * slots, slots)].astype(jnp.float32).reshape(keys, G * (DK + DV))
    at = lax.broadcasted_iota(jnp.int32, (keys, PAD), 0)
    lane = lax.broadcasted_iota(jnp.int32, (keys, PAD), 1)
    spot = (at // 16) % 4
    away = spot + 1 + 4 * lax.rem(part, 2)
    away = jnp.where(part < 2, -away, away)
    away = jnp.where((part == 3) & (spot == 3), 0, away)
    source_z = (z + away + depth) % depth
    source = (at // 64) * (depth * CORES) + source_z * CORES + (at // 8) % CORES
    ids = source * 8 + at % 8
    for group in range(G):
        low = group % 2 == 0
        first = group * DK
        spare = DK if low else 0
        hidden = ((lane == spare) & (ids >= caps[0])) | ((lane == spare + 1) & (ids >= caps[1]))
        bias = jnp.where(hidden, NEG, 0.0)
        window = block[:, first - first % 128 : first - first % 128 + PAD]
        held = jnp.where((lane < DK) if low else (lane >= PAD - DK), window, bias)
        kp[group] = held.astype(jnp.bfloat16)
        vp[group] = block[:, G * DK + group * DV : G * DK + (group + 1) * DV].T.astype(jnp.bfloat16)


def fold(last, tokens, qp, kp, vp, buffers, top, total, held, out_ref):
    per_tile = ROWS // tokens
    tiles = H // G // per_tile

    def scores(group, u):
        rows = pl.ds(pl.multiple_of((group * tiles + u) * ROWS, ROWS), ROWS)
        score = lax.dot_general(kp[group], qp[rows, :], (((1,), (1,)), ((), ())), preferred_element_type=jnp.float32)
        buffers[u][...] = score
        return jnp.broadcast_to(jnp.max(score, axis=0, keepdims=True) * SCALE, (8, ROWS))

    def blend(group, u, best):
        tile = group * tiles + u
        old_top = top[tile]
        new_top = jnp.maximum(old_top, best)
        score = buffers[u][...]
        keys = score.shape[0]
        weight = jnp.exp2(score.reshape(keys // 8, 8, ROWS) * SCALE - new_top[None])
        added = jnp.sum(weight, axis=0)
        value = jnp.dot(vp[group], weight.reshape(keys, ROWS).astype(jnp.bfloat16), preferred_element_type=jnp.float32)
        rescale = jnp.exp2(old_top - new_top)
        added = added + total[tile] * rescale
        value = value + (held[tile].reshape(DV // 8, 8, ROWS) * rescale[None]).reshape(DV, ROWS)
        if last:
            done = (value * (1.0 / jnp.sum(added, axis=0, keepdims=True))).T.astype(jnp.bfloat16)
            for b in range(per_tile):
                head = tile * per_tile + b
                out_ref[:, pl.ds(pl.multiple_of(head * DV, DV), DV)] = done[b * tokens : (b + 1) * tokens]
        else:
            top[tile] = new_top
            total[tile] = added
            held[tile] = value

    def step(group, bests):
        for u in range(tiles):
            at = u + AHEAD
            if at < tiles:
                new = scores(group, at)
            else:
                new = scores(jnp.minimum(group + 1, G - 1), at - tiles)
            blend(group, u, bests[0])
            bests = bests[1:] + (new,)
        return bests

    lax.fori_loop(0, G, step, tuple(scores(0, u) for u in range(AHEAD)))


def slot_of(part, column, spot):
    return ((part * COLS + column) * 4 + spot) * CORES


def kernel(
    depth, q_any, k_any, v_any, limits, valid, out_ref, kv, q_ref, qp, kp, vp, buffers, top, total, held,
    own_sem, z_send, z_recv, x_send, x_recv, d_send, d_recv, ready,
):
    col, z, core = place(depth)
    way = 1 - 2 * core
    mesh_id = pl.DeviceIdType.MESH

    def device(dx, dz, dc):
        target = lax.rem(col + dx, COLS) * (depth * CORES) + lax.rem(z + dz + depth, depth) * CORES
        return {"seq": target + lax.rem(core + dc, CORES)}

    def column(k):
        return lax.rem(col - k + COLS, COLS)

    def push(src, dst, send, recv, target):
        pltpu.make_async_remote_copy(
            src_ref=src, dst_ref=dst, send_sem=send, recv_sem=recv, device_id=target, device_id_type=mesh_id
        ).start()

    def arrived(slab, sem):
        pltpu.make_async_copy(slab, slab, sem).wait()

    def chip(part, column_, spot):
        return kv.at[pl.ds(slot_of(part, column_, spot), CORES)]

    own = slot_of(3, col, 3) + core
    loads = [
        pltpu.make_async_copy(k_any, kv.at[own, :, 0 : G * DK], own_sem.at[0]),
        pltpu.make_async_copy(v_any, kv.at[own, :, G * DK : G * (DK + DV)], own_sem.at[1]),
        pltpu.make_async_copy(q_any, q_ref, own_sem.at[2]),
    ]
    for c in loads:
        c.start()

    barrier = pltpu.get_barrier_semaphore()
    for peer in [device(dx, 0, 0) for dx in (1, 2, 3)] + [device(0, 0, 1)]:
        pl.semaphore_signal(barrier, inc=1, device_id=peer, device_id_type=mesh_id)
    for dz in (1, 2, -1, -2):

        @pl.when(lax.rem(z + dz + depth, depth) > z)
        def _():
            pl.semaphore_signal(barrier, inc=1, device_id=device(0, dz, 0), device_id_type=mesh_id)

    pl.semaphore_wait(barrier, 4 + jnp.minimum(z, 2) + jnp.maximum(z + 3 - depth, 0))
    for i in (1, 2):

        @pl.when(lax.rem(z - way * i + depth, depth) < z)
        def _():
            pl.semaphore_signal(ready.at[i - 1], inc=1, device_id=device(0, -way * i, 0), device_id_type=mesh_id)

    loads[0].wait()
    loads[1].wait()
    mine = kv.at[pl.ds(own, 1)]
    push(mine, mine, d_send.at[ROUNDS * COLS], d_recv.at[ROUNDS * COLS], device(0, 0, 1))
    theirs = kv.at[pl.ds(slot_of(3, col, 3) + 1 - core, 1)]
    arrived(theirs, d_recv.at[ROUNDS * COLS])

    def part_of(direction, r):
        return direction * 2 + r // 2

    def onward(r, src, i):
        at = chip(part_of(core, r), col, r % 2 * 2 + i - 1)

        def go():
            push(src, at, z_send.at[r * 2 + i - 1], z_recv.at[r * 2 + i - 1], device(0, way * i, 0))

        if r == ROUNDS - 1 and i == 2:
            pl.when(core == UP)(go)
        else:
            go()

    def held_back(i):
        return (core == DOWN) & (z < i)

    def relay_source(r):
        return chip(3, col, 3) if r == 0 else chip(part_of(core, r - 1), col, (r - 1) % 2 * 2 + 1)

    for i in (2, 1):

        @pl.when((core == UP) & (z + i < depth))
        def _():
            pl.semaphore_wait(ready.at[i - 1], 1)

        @pl.when(jnp.logical_not(held_back(i)))
        def _():
            onward(0, relay_source(0), i)

    for dx in (2, 1, 3):
        slab = chip(3, col, 3)
        push(slab, slab, x_send.at[ROUNDS * 3 + dx - 1], x_recv.at[ROUNDS * 3 + dx - 1], device(dx, 0, 0))

    def sized(direction, r, fn):
        if isinstance(r, int) and r < ROUNDS - 1:
            fn(4)
            return
        short = (direction == DOWN) & (r == ROUNDS - 1)
        pl.when(short)(lambda: fn(2))
        pl.when(jnp.logical_not(short))(lambda: fn(4))

    def slab_of(direction, r, column_, size):
        part = direction * 2 + r // 2
        return kv.at[pl.ds(slot_of(part, column_, lax.rem(r, 2) * 2), size)]

    def chain(r):
        for i in (1, 2):
            at = chip(part_of(core, r), col, r % 2 * 2 + i - 1)
            if r == ROUNDS - 1 and i == 2:
                pl.when(core == UP)(lambda: arrived(at, z_recv.at[r * 2 + 1]))
            else:
                arrived(at, z_recv.at[r * 2 + i - 1])
        if r < ROUNDS - 1:
            for i in (2, 1):
                pl.when(jnp.logical_not(held_back(i)))(lambda: onward(r + 1, relay_source(r + 1), i))

        def spread(size):
            slab = slab_of(core, r, col, size)
            for dx in (2, 1, 3):
                push(slab, slab, x_send.at[r * 3 + dx - 1], x_recv.at[r * 3 + dx - 1], device(dx, 0, 0))
            push(slab, slab, d_send.at[r * COLS], d_recv.at[r * COLS], device(0, 0, 1))

        sized(core, r, spread)

    def pass_on(r):
        for k in (1, 3, 2):

            def one(size):
                slab = slab_of(core, r, column(k), size)
                arrived(slab, x_recv.at[r * 3 + k - 1])
                push(slab, slab, d_send.at[r * COLS + k], d_recv.at[r * COLS + k], device(0, 0, 1))

            sized(core, r, one)

    def from_partner(half):
        for r in (half * 2, half * 2 + 1):
            for k in range(COLS):
                sized(1 - core, r, lambda size: arrived(slab_of(1 - core, r, column(k), size), d_recv.at[r * COLS + k]))

    tokens = q_ref.shape[0]
    usable = jnp.maximum(lax.shift_right_arithmetic(valid[0] - CBLOCK, 4) + 1, 1)
    first_block = lax.axis_index("seq") * (tokens // QB)
    caps = [jnp.minimum(limits[first_block + b], usable) for b in range(tokens // QB)]

    def weigh(part, last=False):
        spread_keys(part, depth, caps, kv, kp, vp)
        fold(last, tokens, qp, kp, vp, buffers, top, total, held, out_ref)

    loads[2].wait()
    spread_queries(q_ref, qp)
    top[...] = jnp.full(top.shape, -1e38, jnp.float32)
    total[...] = jnp.zeros(total.shape, jnp.float32)
    held[...] = jnp.zeros(held.shape, jnp.float32)
    for k in (1, 2, 3):
        arrived(chip(3, column(k), 3), x_recv.at[ROUNDS * 3 + k - 1])

    low_up = (core == UP) & (z < 4)
    high_up = (core == UP) & (z >= 4)
    mine_near, mine_far = core * 2, core * 2 + 1
    other_near, other_far = 2 - core * 2, 3 - core * 2

    @pl.when(low_up)
    def _():
        from_partner(0)
        weigh(other_near)

    chain(0)
    chain(1)
    pass_on(0)

    @pl.when(jnp.logical_not(high_up))
    def _():
        pass_on(1)

        @pl.when(low_up)
        def _():
            from_partner(1)

        weigh(jnp.where(low_up, other_far, mine_near))

    chain(2)
    chain(3)
    for i in (1, 2):

        @pl.when(held_back(i))
        def _():
            pl.semaphore_wait(ready.at[i - 1], 1)
            for r in range(ROUNDS):
                onward(r, relay_source(r), i)

    pl.when(high_up)(lambda: pass_on(1))
    pass_on(2)
    pass_on(3)

    def rest(t, carry):
        part = jnp.where(
            low_up,
            mine_near,
            jnp.where(t == 0, mine_near, jnp.where(t == 1, mine_far, other_near)),
        )

        @pl.when(part == other_near)
        def _():
            from_partner(0)

        weigh(part)
        return carry

    lax.fori_loop(jnp.where(low_up, 2, jnp.where(high_up, 0, 1)), 3, rest, 0)

    @pl.when(jnp.logical_not(low_up))
    def _():
        from_partner(1)

    weigh(jnp.where(low_up, mine_far, other_far), True)

    for r in range(ROUNDS):
        for i in (1, 2):
            at = chip(0, 0, 0)
            if r == ROUNDS - 1 and i == 2:
                pl.when(core == UP)(lambda: arrived(at, z_send.at[r * 2 + 1]))
            else:
                arrived(at, z_send.at[r * 2 + i - 1])

        def left(size):
            slab = kv.at[pl.ds(0, size)]
            for k in range(3):
                arrived(slab, x_send.at[r * 3 + k])
            for k in range(COLS):
                arrived(slab, d_send.at[r * COLS + k])

        sized(core, r, left)
    for k in range(3):
        arrived(chip(0, 0, 0), x_send.at[ROUNDS * 3 + k])
    arrived(mine, d_send.at[ROUNDS * COLS])


def per_device(depth, queries, sum_keys, sum_values, limits, valid_tokens):
    tokens, width = queries.shape
    vmem = pl.BlockSpec(memory_space=pltpu.VMEM)
    smem = pl.BlockSpec(memory_space=pltpu.SMEM)
    anywhere = pl.BlockSpec(memory_space=pl.ANY)
    dma = pltpu.SemaphoreType.DMA
    keys = CORES * COLS * 4 * sum_keys.shape[0]
    rows = H * tokens
    tiles = rows // ROWS
    slots = 4 * CORES * COLS * 4
    return pl.pallas_call(
        functools.partial(kernel, depth),
        out_shape=jax.ShapeDtypeStruct((tokens, H * DV), jnp.bfloat16),
        in_specs=[anywhere, anywhere, anywhere, smem, smem],
        out_specs=vmem,
        scratch_shapes=[
            pltpu.VMEM((slots, sum_keys.shape[0], G * (DK + DV)), jnp.bfloat16),
            pltpu.VMEM((tokens, width), jnp.bfloat16),
            pltpu.VMEM((rows, PAD), jnp.bfloat16),
            pltpu.VMEM((G, keys, PAD), jnp.bfloat16),
            pltpu.VMEM((G, DV, keys), jnp.bfloat16),
            [pltpu.VMEM((keys, ROWS), jnp.float32)] * (tiles // G),
            pltpu.VMEM((tiles, 8, ROWS), jnp.float32),
            pltpu.VMEM((tiles, 8, ROWS), jnp.float32),
            pltpu.VMEM((tiles, DV, ROWS), jnp.float32),
            dma((3,)),
            dma((ROUNDS * 2,)),
            dma((ROUNDS * 2,)),
            dma((ROUNDS * 3 + 3,)),
            dma((ROUNDS * 3 + 3,)),
            dma((ROUNDS * COLS + 1,)),
            dma((ROUNDS * COLS + 1,)),
            pltpu.SemaphoreType.REGULAR((2,)),
        ],
        compiler_params=pltpu.CompilerParams(collective_id=0, has_side_effects=True),
        name="fused",
    )(queries, sum_keys, sum_values, limits, valid_tokens)


def solution(mesh):
    depth = mesh.shape["seq"] // (COLS * CORES)
    placed = (
        P(("grp", "seq"), None),
        P(("grp", "seq"), None),
        P(("grp", "seq"), None),
        P("grp"),
        P("grp"),
    )
    return jax.shard_map(
        functools.partial(per_device, depth),
        mesh=mesh,
        in_specs=placed,
        out_specs=P(("grp", "seq"), None),
        check_vma=False,
    )
```

```python
import functools

import jax
import jax.numpy as jnp
from jax import lax
from jax.experimental import pallas as pl
from jax.experimental.pallas import tpu as pltpu
from jax.sharding import PartitionSpec as P

H = 64
G = 4
DK = 192
DV = 128
STRIDE = 16
CBLOCK = 32
QB = 64

CORES = 2
COLS = 4
ROUNDS = 4
UP, DOWN = 0, 1
PAD = 256
ROWS = 256
AHEAD = 5
VMEM = 28 * 2**20
NEG = -1e30
SCALE = float(DK) ** -0.5 * 1.4426950408889634


def place(depth):
    me = lax.axis_index("seq")
    return me // (depth * CORES), lax.rem(me // CORES, depth), lax.rem(me, CORES)


def spread_queries(q_ref, qp):
    tokens = q_ref.shape[0]
    lane = lax.broadcasted_iota(jnp.int32, (tokens, PAD), 1)
    token = lax.broadcasted_iota(jnp.int32, (tokens, PAD), 0)
    for head in range(H):
        group = head // (H // G)
        low = group % 2 == 0
        first = head * DK
        spare = DK if low else 0
        marks = jnp.where(lane == spare + token // QB, 1.0, 0.0)
        window = q_ref[:, pl.ds(first - first % 128, PAD)].astype(jnp.float32)
        if low != (first % 128 == 0):
            window = pltpu.roll(window, PAD - 64 if low else 64, 1)
        held = jnp.where((lane < DK) if low else (lane >= PAD - DK), window, marks)
        qp[head * tokens : (head + 1) * tokens, :] = held.astype(jnp.bfloat16)


def spread_keys(part, depth, caps, kv, kp, vp):
    col, z, core = place(depth)
    keys = CORES * COLS * 4 * 8
    slots = keys // 8
    block = kv[pl.ds(part * slots, slots)].astype(jnp.float32).reshape(keys, G * (DK + DV))
    at = lax.broadcasted_iota(jnp.int32, (keys, PAD), 0)
    lane = lax.broadcasted_iota(jnp.int32, (keys, PAD), 1)
    spot = (at // 16) % 4
    away = spot + 1 + 4 * lax.rem(part, 2)
    away = jnp.where(part < 2, -away, away)
    away = jnp.where((part == 3) & (spot == 3), 0, away)
    source_z = (z + away + depth) % depth
    source = (at // 64) * (depth * CORES) + source_z * CORES + (at // 8) % CORES
    ids = source * 8 + at % 8
    for group in range(G):
        low = group % 2 == 0
        first = group * DK
        spare = DK if low else 0
        hidden = ((lane == spare) & (ids >= caps[0])) | ((lane == spare + 1) & (ids >= caps[1]))
        bias = jnp.where(hidden, NEG, 0.0)
        window = block[:, first - first % 128 : first - first % 128 + PAD]
        held = jnp.where((lane < DK) if low else (lane >= PAD - DK), window, bias)
        kp[group] = held.astype(jnp.bfloat16)
        vp[group] = block[:, G * DK + group * DV : G * DK + (group + 1) * DV].T.astype(jnp.bfloat16)


def fold(last, tokens, qp, kp, vp, buffers, top, total, held, out_ref, leave):
    per_tile = ROWS // tokens
    tiles = H // G // per_tile

    def scores(group, u):
        rows = pl.ds(pl.multiple_of((group * tiles + u) * ROWS, ROWS), ROWS)
        score = lax.dot_general(kp[group], qp[rows, :], (((1,), (1,)), ((), ())), preferred_element_type=jnp.float32)
        buffers[u][...] = score
        return jnp.broadcast_to(jnp.max(score, axis=0, keepdims=True) * SCALE, (8, ROWS))

    def blend(group, u, best):
        tile = group * tiles + u
        old_top = top[tile]
        new_top = jnp.maximum(old_top, best)
        score = buffers[u][...]
        keys = score.shape[0]
        weight = jnp.exp2(score.reshape(keys // 8, 8, ROWS) * SCALE - new_top[None])
        added = jnp.sum(weight, axis=0)
        value = jnp.dot(vp[group], weight.reshape(keys, ROWS).astype(jnp.bfloat16), preferred_element_type=jnp.float32)
        rescale = jnp.exp2(old_top - new_top)
        added = added + total[tile] * rescale
        value = value + (held[tile].reshape(DV // 8, 8, ROWS) * rescale[None]).reshape(DV, ROWS)
        if last:
            done = (value * (1.0 / jnp.sum(added, axis=0, keepdims=True))).T.astype(jnp.bfloat16)
            for b in range(per_tile):
                head = tile * per_tile + b
                out_ref[:, pl.ds(pl.multiple_of(head * DV, DV), DV)] = done[b * tokens : (b + 1) * tokens]
        else:
            top[tile] = new_top
            total[tile] = added
            held[tile] = value

    def step(group, bests):
        for u in range(tiles):
            at = u + AHEAD
            if at < tiles:
                new = scores(group, at)
            else:
                new = scores(jnp.minimum(group + 1, G - 1), at - tiles)
            blend(group, u, bests[0])
            bests = bests[1:] + (new,)
        if last:
            leave(group).start()
        return bests

    lax.fori_loop(0, G, step, tuple(scores(0, u) for u in range(AHEAD)))


def slot_of(part, column, spot):
    return ((part * COLS + column) * 4 + spot) * CORES


def kernel(
    depth, q_any, k_any, v_any, limits, valid, out_any, kv, q_ref, out_ref, qp, kp, vp, buffers, top, total, held,
    own_sem, out_sem, z_send, z_recv, x_send, x_recv, d_send, d_recv, ready,
):
    col, z, core = place(depth)
    way = 1 - 2 * core
    mesh_id = pl.DeviceIdType.MESH

    def device(dx, dz, dc):
        target = lax.rem(col + dx, COLS) * (depth * CORES) + lax.rem(z + dz + depth, depth) * CORES
        return {"seq": target + lax.rem(core + dc, CORES)}

    def column(k):
        return lax.rem(col - k + COLS, COLS)

    def push(src, dst, send, recv, target):
        pltpu.make_async_remote_copy(
            src_ref=src, dst_ref=dst, send_sem=send, recv_sem=recv, device_id=target, device_id_type=mesh_id
        ).start()

    def arrived(slab, sem):
        pltpu.make_async_copy(slab, slab, sem).wait()

    def chip(part, column_, spot):
        return kv.at[pl.ds(slot_of(part, column_, spot), CORES)]

    own = slot_of(3, col, 3) + core
    loads = [
        pltpu.make_async_copy(k_any, kv.at[own, :, 0 : G * DK], own_sem.at[0]),
        pltpu.make_async_copy(v_any, kv.at[own, :, G * DK : G * (DK + DV)], own_sem.at[1]),
        pltpu.make_async_copy(q_any, q_ref, own_sem.at[2]),
    ]
    for c in loads:
        c.start()

    first_chip = (col == 0) & (z == 0)

    def turn(at_z):
        return jnp.where((col == 0) & (core == 0) & (at_z == 0), depth, at_z)

    def along(dz):
        return turn(lax.rem(z + dz + depth, depth))

    barrier = pltpu.get_barrier_semaphore()

    def greet(peer):
        pl.semaphore_signal(barrier, inc=1, device_id=peer, device_id_type=mesh_id)

    for dx in (1, 2, 3):
        pl.when(col >= dx)(lambda: greet(device(COLS - dx, 0, 0)))
    pl.when(col == COLS - 2)(lambda: greet(device(1, 0, 0)))
    pl.when(jnp.logical_not(first_chip) | (core == 1))(lambda: greet(device(0, 0, 1)))
    my_turn = turn(z)
    expected = jnp.where(col == COLS - 1, 1, COLS - 1 - col) + jnp.where(first_chip & (core == 1), 0, 1)
    for dz in (1, 2, -1, -2):
        pl.when(along(dz) > my_turn)(lambda: greet(device(0, dz, 0)))
        expected = expected + jnp.where(along(dz) < my_turn, 1, 0)
    pl.semaphore_wait(barrier, expected)

    def answer(i, peer):
        pl.semaphore_signal(ready.at[i], inc=1, device_id=peer, device_id_type=mesh_id)

    for i in (1, 2):
        pl.when(along(-way * i) < my_turn)(lambda: answer(i - 1, device(0, -way * i, 0)))
    pl.when(first_chip & (core == 0))(lambda: answer(2, device(0, 0, 1)))

    loads[0].wait()
    loads[1].wait()
    mine = kv.at[pl.ds(own, 1)]
    theirs = kv.at[pl.ds(slot_of(3, col, 3) + 1 - core, 1)]

    def share():
        push(mine, mine, d_send.at[ROUNDS * COLS], d_recv.at[ROUNDS * COLS], device(0, 0, 1))
        arrived(theirs, d_recv.at[ROUNDS * COLS])

    def part_of(direction, r):
        return direction * 2 + r // 2

    def onward(r, src, i):
        at = chip(part_of(core, r), col, r % 2 * 2 + i - 1)

        def go():
            push(src, at, z_send.at[r * 2 + i - 1], z_recv.at[r * 2 + i - 1], device(0, way * i, 0))

        if r == ROUNDS - 1 and i == 2:
            pl.when(core == UP)(go)
        else:
            go()

    def held_back(i):
        return (core == DOWN) & (z < i)

    def relay_source(r):
        return chip(3, col, 3) if r == 0 else chip(part_of(core, r - 1), col, (r - 1) % 2 * 2 + 1)

    def across(r, slab):
        two = (col == 1) | (col == 0) if r == ROUNDS else (col == 1) | ((col == 0) & jnp.logical_not(over))
        for dx, to in ((3, col == 0), (2, two), (1, col < COLS - 1)):

            @pl.when(to)
            def _():
                push(slab, slab, x_send.at[r * 3 + dx - 1], x_recv.at[r * 3 + dx - 1], device(dx, 0, 0))

    over = z >= depth // 2
    last_to_share = first_chip & (core == 1)

    @pl.when(jnp.logical_not(last_to_share))
    def _():
        share()
        for i in (2, 1):

            @pl.when((core == UP) & (along(i) > my_turn))
            def _():
                pl.semaphore_wait(ready.at[i - 1], 1)

            pl.when(jnp.logical_not(held_back(i)))(lambda: onward(0, relay_source(0), i))

        across(ROUNDS, chip(3, col, 3))

    def from_across(r, k, slab):
        arrived(slab, x_recv.at[r * 3 + k - 1])
        if k == 3 and r < ROUNDS:

            @pl.when(over)
            def _():
                push(slab, slab, x_send.at[r * 3 + 2], x_recv.at[r * 3 + 1], device(3, 0, 0))

    def sized(direction, r, fn):
        if isinstance(r, int) and r < ROUNDS - 1:
            fn(4)
            return
        short = (direction == DOWN) & (r == ROUNDS - 1)
        pl.when(short)(lambda: fn(2))
        pl.when(jnp.logical_not(short))(lambda: fn(4))

    def slab_of(direction, r, column_, size):
        part = direction * 2 + r // 2
        return kv.at[pl.ds(slot_of(part, column_, lax.rem(r, 2) * 2), size)]

    paired = (core == UP) | (z > 0)

    def chain(r):
        for i in (1, 2):
            at = chip(part_of(core, r), col, r % 2 * 2 + i - 1)
            if r == ROUNDS - 1 and i == 2:
                pl.when(core == UP)(lambda: arrived(at, z_recv.at[r * 2 + 1]))
            else:
                arrived(at, z_recv.at[r * 2 + i - 1])
        if r < ROUNDS - 1:
            for i in (2, 1):
                pl.when(jnp.logical_not(held_back(i)))(lambda: onward(r + 1, relay_source(r + 1), i))

        def spread(size):
            slab = slab_of(core, r, col, size)
            across(r, slab)

            @pl.when(paired)
            def _():
                push(slab, slab, d_send.at[r * COLS], d_recv.at[r * COLS], device(0, 0, 1))

        sized(core, r, spread)

    def pass_on(r):
        for k in (3, 1, 2):

            def one(size):
                slab = slab_of(core, r, column(k), size)
                from_across(r, k, slab)
                push(slab, slab, d_send.at[r * COLS + k], d_recv.at[r * COLS + k], device(0, 0, 1))

            pl.when(k <= col)(lambda: sized(core, r, one))

    def from_partner(half):
        for r in (half * 2, half * 2 + 1):
            for k in range(COLS):

                @pl.when((k <= col) & ((core == DOWN) | (z > 0)) if k == 0 else k <= col)
                def _():
                    sized(
                        1 - core, r, lambda size: arrived(slab_of(1 - core, r, column(k), size), d_recv.at[r * COLS + k])
                    )

    tokens = q_ref.shape[0]
    usable = jnp.maximum(lax.shift_right_arithmetic(valid[0] - CBLOCK, 4) + 1, 1)
    first_block = lax.axis_index("seq") * (tokens // QB)
    caps = [jnp.minimum(limits[first_block + b], usable) for b in range(tokens // QB)]

    def weigh(part, last=False):
        spread_keys(part, depth, caps, kv, kp, vp)
        fold(last, tokens, qp, kp, vp, buffers, top, total, held, out_ref, leave)

    def leave(group):
        heads = pl.ds(pl.multiple_of(group * (H // G * DV), 128), H // G * DV)
        return pltpu.make_async_copy(out_ref.at[:, heads], out_any.at[:, heads], out_sem.at[group])

    def prep():
        loads[2].wait()
        spread_queries(q_ref, qp)
        top[...] = jnp.full(top.shape, -1e38, jnp.float32)
        total[...] = jnp.zeros(total.shape, jnp.float32)
        held[...] = jnp.zeros(held.shape, jnp.float32)
        for column_ in range(1, COLS):

            @pl.when(column_ > col)
            def _():
                for part in range(4):
                    unused = kv.at[pl.ds(slot_of(part, column_, 0), 4 * CORES)]
                    unused[...] = jnp.zeros(unused.shape, unused.dtype)

        @pl.when((core == UP) & (z == 0))
        def _():
            for unused in (kv.at[pl.ds(slot_of(2, col, 0), 4 * CORES)], kv.at[pl.ds(slot_of(3, col, 0), 3 * CORES)]):
                unused[...] = jnp.zeros(unused.shape, unused.dtype)

    def same_z():
        for k in (3, 1, 2):
            pl.when(k <= col)(lambda: from_across(ROUNDS, k, chip(3, column(k), 3)))

    up = core == UP
    early = jnp.where(up, jnp.minimum(z // 2, ROUNDS), 0)
    low_up = up & (early < ROUNDS)
    high_up = up & (early == ROUNDS)
    near_late = up & (early < 2)
    mine_near, mine_far = core * 2, core * 2 + 1
    other_near, other_far = 2 - core * 2, 3 - core * 2

    for r in range(ROUNDS):

        @pl.when(r < early)
        def _():
            chain(r)
            if r >= 1:
                pass_on(r - 1)

    prep()

    @pl.when(low_up)
    def _():
        from_partner(0)
        weigh(other_near)

    @pl.when(early < 2)
    def _():
        pl.when(early < 1)(lambda: chain(0))
        chain(1)
        pass_on(0)

    pl.when(jnp.logical_not(near_late))(lambda: pl.when(early < 3)(lambda: pass_on(1)))
    @pl.when(near_late)
    def _():
        same_z()
        from_partner(1)

    weigh(jnp.where(near_late, other_far, mine_near))

    def hold():
        @pl.when(last_to_share)
        def _():
            pl.semaphore_wait(ready.at[2], 1)
            share()
            across(ROUNDS, chip(3, col, 3))

        for i in (1, 2):

            @pl.when(held_back(i))
            def _():
                pl.semaphore_wait(ready.at[i - 1], 1)
                for r in range(ROUNDS):
                    onward(r, relay_source(r), i)

    @pl.when(early < 3)
    def _():
        chain(2)
        pl.when(near_late)(lambda: pass_on(1))

    hold()
    pl.when(jnp.logical_not(near_late))(same_z)

    between = low_up & jnp.logical_not(near_late)

    @pl.when(between)
    def _():
        from_partner(1)
        weigh(other_far)

    @pl.when(early < ROUNDS)
    def _():
        chain(ROUNDS - 1)
        pl.when(early < 3)(lambda: pass_on(2))

    pl.when(near_late)(lambda: weigh(mine_near))
    pl.when(early == 3)(lambda: pass_on(2))
    pass_on(3)

    def rest(t, carry):
        part = jnp.where((t == 0) == up, other_near, mine_far)
        pl.when(part == other_near)(lambda: from_partner(0))
        weigh(part)
        return carry

    lax.fori_loop(0, jnp.where(low_up, 0, 2), rest, 0)
    pl.when(jnp.logical_not(low_up))(lambda: from_partner(1))
    weigh(jnp.where(low_up, mine_far, other_far), True)
    for group in range(G):
        leave(group).wait()

    def across_left(r, slab):
        two = (col == 1) | (col == 0) if r == ROUNDS else (col == 1) | ((col == 0) & jnp.logical_not(over))
        three = (col == 0) if r == ROUNDS else (col == 0) | ((col == COLS - 1) & over)
        for dx, to in ((1, col < COLS - 1), (2, two), (3, three)):
            pl.when(to)(lambda: arrived(slab, x_send.at[r * 3 + dx - 1]))

    for r in range(ROUNDS):
        for i in (1, 2):
            at = chip(0, 0, 0)
            if r == ROUNDS - 1 and i == 2:
                pl.when(core == UP)(lambda: arrived(at, z_send.at[r * 2 + 1]))
            else:
                arrived(at, z_send.at[r * 2 + i - 1])

        def left(size):
            slab = kv.at[pl.ds(0, size)]
            across_left(r, slab)
            for k in range(COLS):
                pl.when((k <= col) & paired if k == 0 else k <= col)(lambda: arrived(slab, d_send.at[r * COLS + k]))

        sized(core, r, left)
    across_left(ROUNDS, chip(0, 0, 0))
    arrived(mine, d_send.at[ROUNDS * COLS])


def per_device(depth, queries, sum_keys, sum_values, limits, valid_tokens):
    tokens, width = queries.shape
    smem = pl.BlockSpec(memory_space=pltpu.SMEM)
    anywhere = pl.BlockSpec(memory_space=pl.ANY)
    main = pl.BlockSpec(memory_space=pltpu.HBM)
    dma = pltpu.SemaphoreType.DMA
    keys = CORES * COLS * 4 * sum_keys.shape[0]
    rows = H * tokens
    tiles = rows // ROWS
    slots = 4 * CORES * COLS * 4
    return pl.pallas_call(
        functools.partial(kernel, depth),
        out_shape=jax.ShapeDtypeStruct((tokens, H * DV), jnp.bfloat16),
        in_specs=[main, main, main, smem, smem],
        out_specs=anywhere,
        scratch_shapes=[
            pltpu.VMEM((slots, sum_keys.shape[0], G * (DK + DV)), jnp.bfloat16),
            pltpu.VMEM((tokens, width), jnp.bfloat16),
            pltpu.VMEM((tokens, H * DV), jnp.bfloat16),
            pltpu.VMEM((rows, PAD), jnp.bfloat16),
            pltpu.VMEM((G, keys, PAD), jnp.bfloat16),
            pltpu.VMEM((G, DV, keys), jnp.bfloat16),
            [pltpu.VMEM((keys, ROWS), jnp.float32)] * (tiles // G),
            pltpu.VMEM((tiles, 8, ROWS), jnp.float32),
            pltpu.VMEM((tiles, 8, ROWS), jnp.float32),
            pltpu.VMEM((tiles, DV, ROWS), jnp.float32),
            dma((3,)),
            dma((G,)),
            dma((ROUNDS * 2,)),
            dma((ROUNDS * 2,)),
            dma((ROUNDS * 3 + 3,)),
            dma((ROUNDS * 3 + 3,)),
            dma((ROUNDS * COLS + 1,)),
            dma((ROUNDS * COLS + 1,)),
            pltpu.SemaphoreType.REGULAR((3,)),
        ],
        compiler_params=pltpu.CompilerParams(collective_id=0, has_side_effects=True, vmem_limit_bytes=VMEM),
        name="fused",
    )(queries, sum_keys, sum_values, limits, valid_tokens)


def solution(mesh):
    depth = mesh.shape["seq"] // (COLS * CORES)
    placed = (
        P(("grp", "seq"), None),
        P(("grp", "seq"), None),
        P(("grp", "seq"), None),
        P("grp"),
        P("grp"),
    )
    return jax.shard_map(
        functools.partial(per_device, depth),
        mesh=mesh,
        in_specs=placed,
        out_specs=P(("grp", "seq"), None),
        check_vma=False,
    )
```

```python
import functools

import jax
import jax.numpy as jnp
from jax import lax
from jax.experimental import pallas as pl
from jax.experimental.pallas import tpu as pltpu
from jax.sharding import PartitionSpec as P

H = 64
G = 4
DK = 192
DV = 128
STRIDE = 16
CBLOCK = 32
QB = 64

CORES = 2
COLS = 4
ROUNDS = 4
UP, DOWN = 0, 1
PAD = 256
ROWS = 256
AHEAD = 5
VMEM = 61 * 2**20
NEG = -1e30
SCALE = float(DK) ** -0.5 * 1.4426950408889634


def place(depth):
    me = lax.axis_index("seq")
    return me // (depth * CORES), lax.rem(me // CORES, depth), lax.rem(me, CORES)


def spread_queries(q_ref, qp):
    tokens = q_ref.shape[0]
    lane = lax.broadcasted_iota(jnp.int32, (tokens, PAD), 1)
    token = lax.broadcasted_iota(jnp.int32, (tokens, PAD), 0)
    for head in range(H):
        group = head // (H // G)
        low = group % 2 == 0
        first = head * DK
        spare = DK if low else 0
        marks = jnp.where(lane == spare + token // QB, 1.0, 0.0)
        window = q_ref[:, pl.ds(first - first % 128, PAD)].astype(jnp.float32)
        if low != (first % 128 == 0):
            window = pltpu.roll(window, PAD - 64 if low else 64, 1)
        held = jnp.where((lane < DK) if low else (lane >= PAD - DK), window, marks)
        qp[head * tokens : (head + 1) * tokens, :] = held.astype(jnp.bfloat16)


def spread_keys(part, depth, caps, kv, kp, vp):
    col, z, core = place(depth)
    keys = CORES * COLS * 4 * 8
    slots = keys // 8
    block = kv[pl.ds(part * slots, slots)].astype(jnp.float32).reshape(keys, G * (DK + DV))
    at = lax.broadcasted_iota(jnp.int32, (keys, PAD), 0)
    lane = lax.broadcasted_iota(jnp.int32, (keys, PAD), 1)
    spot = (at // 16) % 4
    away = spot + 1 + 4 * lax.rem(part, 2)
    away = jnp.where(part < 2, -away, away)
    away = jnp.where((part == 3) & (spot == 3), 0, away)
    source_z = (z + away + depth) % depth
    source = (at // 64) * (depth * CORES) + source_z * CORES + (at // 8) % CORES
    ids = source * 8 + at % 8
    for group in range(G):
        low = group % 2 == 0
        first = group * DK
        spare = DK if low else 0
        hidden = ((lane == spare) & (ids >= caps[0])) | ((lane == spare + 1) & (ids >= caps[1]))
        bias = jnp.where(hidden, NEG, 0.0)
        window = block[:, first - first % 128 : first - first % 128 + PAD]
        held = jnp.where((lane < DK) if low else (lane >= PAD - DK), window, bias)
        kp[group] = held.astype(jnp.bfloat16)
        vp[group] = block[:, G * DK + group * DV : G * DK + (group + 1) * DV].T.astype(jnp.bfloat16)


def fold(last, tokens, qp, kp, vp, buffers, top, total, held, out_ref, leave):
    per_tile = ROWS // tokens
    tiles = H // G // per_tile

    def scores(group, u):
        rows = pl.ds(pl.multiple_of((group * tiles + u) * ROWS, ROWS), ROWS)
        score = lax.dot_general(kp[group], qp[rows, :], (((1,), (1,)), ((), ())), preferred_element_type=jnp.float32)
        buffers[u][...] = score
        return jnp.broadcast_to(jnp.max(score, axis=0, keepdims=True) * SCALE, (8, ROWS))

    def blend(group, u, best):
        tile = group * tiles + u
        old_top = top[tile]
        new_top = jnp.maximum(old_top, best)
        score = buffers[u][...]
        keys = score.shape[0]
        weight = jnp.exp2(score.reshape(keys // 8, 8, ROWS) * SCALE - new_top[None])
        added = jnp.sum(weight, axis=0)
        value = jnp.dot(vp[group], weight.reshape(keys, ROWS).astype(jnp.bfloat16), preferred_element_type=jnp.float32)
        rescale = jnp.exp2(old_top - new_top)
        added = added + total[tile] * rescale
        value = value + (held[tile].reshape(DV // 8, 8, ROWS) * rescale[None]).reshape(DV, ROWS)
        if last:
            done = (value * (1.0 / jnp.sum(added, axis=0, keepdims=True))).T.astype(jnp.bfloat16)
            for b in range(per_tile):
                head = tile * per_tile + b
                out_ref[:, pl.ds(pl.multiple_of(head * DV, DV), DV)] = done[b * tokens : (b + 1) * tokens]
        else:
            top[tile] = new_top
            total[tile] = added
            held[tile] = value

    def step(group, bests):
        for u in range(tiles):
            at = u + AHEAD
            if at < tiles:
                new = scores(group, at)
            else:
                new = scores(jnp.minimum(group + 1, G - 1), at - tiles)
            blend(group, u, bests[0])
            bests = bests[1:] + (new,)
        if last:
            leave(group).start()
        return bests

    lax.fori_loop(0, G, step, tuple(scores(0, u) for u in range(AHEAD)))


def slot_of(part, column, spot):
    return ((part * COLS + column) * 4 + spot) * CORES


def kernel(
    depth, q_any, k_any, v_any, limits, valid, out_any, kv, q_ref, out_ref, qp, kp, vp, buffers, top, total, held,
    own_sem, out_sem, z_send, z_recv, x_send, x_recv, d_send, d_recv, ready,
):
    col, z, core = place(depth)
    way = 1 - 2 * core
    mesh_id = pl.DeviceIdType.MESH

    def device(dx, dz, dc):
        target = lax.rem(col + dx, COLS) * (depth * CORES) + lax.rem(z + dz + depth, depth) * CORES
        return {"seq": target + lax.rem(core + dc, CORES)}

    def column(k):
        return lax.rem(col - k + COLS, COLS)

    def push(src, dst, send, recv, target):
        pltpu.make_async_remote_copy(
            src_ref=src, dst_ref=dst, send_sem=send, recv_sem=recv, device_id=target, device_id_type=mesh_id
        ).start()

    def arrived(slab, sem):
        pltpu.make_async_copy(slab, slab, sem).wait()

    def chip(part, column_, spot):
        return kv.at[pl.ds(slot_of(part, column_, spot), CORES)]

    own = slot_of(3, col, 3) + core
    loads = [
        pltpu.make_async_copy(k_any, kv.at[own, :, 0 : G * DK], own_sem.at[0]),
        pltpu.make_async_copy(v_any, kv.at[own, :, G * DK : G * (DK + DV)], own_sem.at[1]),
        pltpu.make_async_copy(q_any, q_ref, own_sem.at[2]),
    ]
    for c in loads:
        c.start()

    first_chip = (col == 0) & (z == 0)

    def turn(at_z):
        return jnp.where((col == 0) & (core == 0) & (at_z == 0), depth, at_z)

    def along(dz):
        return turn(lax.rem(z + dz + depth, depth))

    barrier = pltpu.get_barrier_semaphore()

    def greet(peer):
        pl.semaphore_signal(barrier, inc=1, device_id=peer, device_id_type=mesh_id)

    for dx in (1, 2, 3):
        pl.when(col >= dx)(lambda: greet(device(COLS - dx, 0, 0)))
    pl.when(col == COLS - 2)(lambda: greet(device(1, 0, 0)))
    pl.when(jnp.logical_not(first_chip) | (core == 1))(lambda: greet(device(0, 0, 1)))
    my_turn = turn(z)
    expected = jnp.where(col == COLS - 1, 1, COLS - 1 - col) + jnp.where(first_chip & (core == 1), 0, 1)
    for dz in (1, 2, -1, -2):
        pl.when(along(dz) > my_turn)(lambda: greet(device(0, dz, 0)))
        expected = expected + jnp.where(along(dz) < my_turn, 1, 0)
    pl.semaphore_wait(barrier, expected)

    def answer(i, peer):
        pl.semaphore_signal(ready.at[i], inc=1, device_id=peer, device_id_type=mesh_id)

    for i in (1, 2):
        pl.when(along(-way * i) < my_turn)(lambda: answer(i - 1, device(0, -way * i, 0)))
    pl.when(first_chip & (core == 0))(lambda: answer(2, device(0, 0, 1)))

    loads[0].wait()
    loads[1].wait()
    mine = kv.at[pl.ds(own, 1)]
    theirs = kv.at[pl.ds(slot_of(3, col, 3) + 1 - core, 1)]

    def share():
        push(mine, mine, d_send.at[ROUNDS * COLS], d_recv.at[ROUNDS * COLS], device(0, 0, 1))
        arrived(theirs, d_recv.at[ROUNDS * COLS])

    def part_of(direction, r):
        return direction * 2 + r // 2

    def onward(r, src, i):
        at = chip(part_of(core, r), col, r % 2 * 2 + i - 1)

        def go():
            push(src, at, z_send.at[r * 2 + i - 1], z_recv.at[r * 2 + i - 1], device(0, way * i, 0))

        if r == ROUNDS - 1 and i == 2:
            pl.when(core == UP)(go)
        else:
            go()

    def held_back(i):
        return (core == DOWN) & (z < i)

    def relay_source(r):
        return chip(3, col, 3) if r == 0 else chip(part_of(core, r - 1), col, (r - 1) % 2 * 2 + 1)

    def across(r, slab):
        two = (col == 1) | (col == 0) if r == ROUNDS else (col == 1) | ((col == 0) & jnp.logical_not(over))
        for dx, to in ((3, col == 0), (2, two), (1, col < COLS - 1)):

            @pl.when(to)
            def _():
                push(slab, slab, x_send.at[r * 3 + dx - 1], x_recv.at[r * 3 + dx - 1], device(dx, 0, 0))

    over = z >= depth // 2
    last_to_share = first_chip & (core == 1)

    @pl.when(jnp.logical_not(last_to_share))
    def _():
        share()
        for i in (2, 1):

            @pl.when((core == UP) & (along(i) > my_turn))
            def _():
                pl.semaphore_wait(ready.at[i - 1], 1)

            pl.when(jnp.logical_not(held_back(i)))(lambda: onward(0, relay_source(0), i))

        across(ROUNDS, chip(3, col, 3))

    def from_across(r, k, slab):
        arrived(slab, x_recv.at[r * 3 + k - 1])
        if k == 3 and r < ROUNDS:

            @pl.when(over)
            def _():
                push(slab, slab, x_send.at[r * 3 + 2], x_recv.at[r * 3 + 1], device(3, 0, 0))

    def sized(direction, r, fn):
        if isinstance(r, int) and r < ROUNDS - 1:
            fn(4)
            return
        short = (direction == DOWN) & (r == ROUNDS - 1)
        pl.when(short)(lambda: fn(2))
        pl.when(jnp.logical_not(short))(lambda: fn(4))

    def slab_of(direction, r, column_, size):
        part = direction * 2 + r // 2
        return kv.at[pl.ds(slot_of(part, column_, lax.rem(r, 2) * 2), size)]

    paired = (core == UP) | (z > 0)

    def chain(r):
        for i in (1, 2):
            at = chip(part_of(core, r), col, r % 2 * 2 + i - 1)
            if r == ROUNDS - 1 and i == 2:
                pl.when(core == UP)(lambda: arrived(at, z_recv.at[r * 2 + 1]))
            else:
                arrived(at, z_recv.at[r * 2 + i - 1])
        if r < ROUNDS - 1:
            for i in (2, 1):
                pl.when(jnp.logical_not(held_back(i)))(lambda: onward(r + 1, relay_source(r + 1), i))

        def spread(size):
            slab = slab_of(core, r, col, size)
            across(r, slab)

            @pl.when(paired)
            def _():
                push(slab, slab, d_send.at[r * COLS], d_recv.at[r * COLS], device(0, 0, 1))

        sized(core, r, spread)

    def pass_on(r):
        for k in (3, 1, 2):

            def one(size):
                slab = slab_of(core, r, column(k), size)
                from_across(r, k, slab)
                push(slab, slab, d_send.at[r * COLS + k], d_recv.at[r * COLS + k], device(0, 0, 1))

            pl.when(k <= col)(lambda: sized(core, r, one))

    def from_partner(half):
        for r in (half * 2, half * 2 + 1):
            for k in range(COLS):

                @pl.when((k <= col) & ((core == DOWN) | (z > 0)) if k == 0 else k <= col)
                def _():
                    sized(
                        1 - core, r, lambda size: arrived(slab_of(1 - core, r, column(k), size), d_recv.at[r * COLS + k])
                    )

    tokens = q_ref.shape[0]
    usable = jnp.maximum(lax.shift_right_arithmetic(valid[0] - CBLOCK, 4) + 1, 1)
    first_block = lax.axis_index("seq") * (tokens // QB)
    caps = [jnp.minimum(limits[first_block + b], usable) for b in range(tokens // QB)]

    def weigh(part, last=False):
        spread_keys(part, depth, caps, kv, kp, vp)
        fold(last, tokens, qp, kp, vp, buffers, top, total, held, out_ref, leave)

    def leave(group):
        heads = pl.ds(pl.multiple_of(group * (H // G * DV), 128), H // G * DV)
        return pltpu.make_async_copy(out_ref.at[:, heads], out_any.at[:, heads], out_sem.at[group])

    def prep():
        loads[2].wait()
        spread_queries(q_ref, qp)
        top[...] = jnp.full(top.shape, -1e38, jnp.float32)
        total[...] = jnp.zeros(total.shape, jnp.float32)
        held[...] = jnp.zeros(held.shape, jnp.float32)
        for column_ in range(1, COLS):

            @pl.when(column_ > col)
            def _():
                for part in range(4):
                    unused = kv.at[pl.ds(slot_of(part, column_, 0), 4 * CORES)]
                    unused[...] = jnp.zeros(unused.shape, unused.dtype)

        @pl.when((core == UP) & (z == 0))
        def _():
            for unused in (kv.at[pl.ds(slot_of(2, col, 0), 4 * CORES)], kv.at[pl.ds(slot_of(3, col, 0), 3 * CORES)]):
                unused[...] = jnp.zeros(unused.shape, unused.dtype)

    def same_z():
        for k in (3, 1, 2):
            pl.when(k <= col)(lambda: from_across(ROUNDS, k, chip(3, column(k), 3)))

    up = core == UP
    early = jnp.where(up, jnp.minimum(z // 2, ROUNDS), 0)
    low_up = up & (early < ROUNDS)
    high_up = up & (early == ROUNDS)
    near_late = up & (early < 2)
    mine_near, mine_far = core * 2, core * 2 + 1
    other_near, other_far = 2 - core * 2, 3 - core * 2

    for r in range(ROUNDS):

        @pl.when(r < early)
        def _():
            chain(r)

        if r == ROUNDS - 2:

            @pl.when(early >= 2)
            def _():
                pass_on(0)
                pl.when(early >= 3)(lambda: pass_on(1))

        if r == ROUNDS - 1:
            pl.when(early == ROUNDS)(lambda: pass_on(2))

    prep()

    @pl.when(low_up)
    def _():
        from_partner(0)
        weigh(other_near)

    @pl.when(early < 2)
    def _():
        pl.when(early < 1)(lambda: chain(0))
        chain(1)
        pass_on(0)

    pl.when(jnp.logical_not(near_late))(lambda: pl.when(early < 3)(lambda: pass_on(1)))
    @pl.when(near_late)
    def _():
        same_z()
        from_partner(1)

    weigh(jnp.where(near_late, other_far, mine_near))

    def hold():
        @pl.when(last_to_share)
        def _():
            pl.semaphore_wait(ready.at[2], 1)
            share()
            across(ROUNDS, chip(3, col, 3))

        for i in (1, 2):

            @pl.when(held_back(i))
            def _():
                pl.semaphore_wait(ready.at[i - 1], 1)
                for r in range(ROUNDS):
                    onward(r, relay_source(r), i)

    @pl.when(early < 3)
    def _():
        chain(2)
        pl.when(near_late)(lambda: pass_on(1))

    hold()
    pl.when(jnp.logical_not(near_late))(same_z)

    between = low_up & jnp.logical_not(near_late)

    @pl.when(between)
    def _():
        from_partner(1)
        weigh(other_far)

    @pl.when(early < ROUNDS)
    def _():
        chain(ROUNDS - 1)
        pl.when(early < 3)(lambda: pass_on(2))

    pl.when(near_late)(lambda: weigh(mine_near))
    pl.when(early == 3)(lambda: pass_on(2))
    pass_on(3)

    def rest(t, carry):
        part = jnp.where((t == 0) == up, other_near, mine_far)
        pl.when(part == other_near)(lambda: from_partner(0))
        weigh(part)
        return carry

    lax.fori_loop(0, jnp.where(low_up, 0, 2), rest, 0)
    pl.when(jnp.logical_not(low_up))(lambda: from_partner(1))
    weigh(jnp.where(low_up, mine_far, other_far), True)
    for group in range(G):
        leave(group).wait()

    def across_left(r, slab):
        two = (col == 1) | (col == 0) if r == ROUNDS else (col == 1) | ((col == 0) & jnp.logical_not(over))
        three = (col == 0) if r == ROUNDS else (col == 0) | ((col == COLS - 1) & over)
        for dx, to in ((1, col < COLS - 1), (2, two), (3, three)):
            pl.when(to)(lambda: arrived(slab, x_send.at[r * 3 + dx - 1]))

    for r in range(ROUNDS):
        for i in (1, 2):
            at = chip(0, 0, 0)
            if r == ROUNDS - 1 and i == 2:
                pl.when(core == UP)(lambda: arrived(at, z_send.at[r * 2 + 1]))
            else:
                arrived(at, z_send.at[r * 2 + i - 1])

        def left(size):
            slab = kv.at[pl.ds(0, size)]
            across_left(r, slab)
            for k in range(COLS):
                pl.when((k <= col) & paired if k == 0 else k <= col)(lambda: arrived(slab, d_send.at[r * COLS + k]))

        sized(core, r, left)
    across_left(ROUNDS, chip(0, 0, 0))
    arrived(mine, d_send.at[ROUNDS * COLS])


def per_device(depth, queries, sum_keys, sum_values, limits, valid_tokens):
    tokens, width = queries.shape
    smem = pl.BlockSpec(memory_space=pltpu.SMEM)
    anywhere = pl.BlockSpec(memory_space=pl.ANY)
    main = pl.BlockSpec(memory_space=pltpu.HBM)
    dma = pltpu.SemaphoreType.DMA
    keys = CORES * COLS * 4 * sum_keys.shape[0]
    rows = H * tokens
    tiles = rows // ROWS
    slots = 4 * CORES * COLS * 4
    return pl.pallas_call(
        functools.partial(kernel, depth),
        out_shape=pltpu.VMEM((tokens, H * DV), jnp.bfloat16),
        in_specs=[main, main, main, smem, smem],
        out_specs=anywhere,
        scratch_shapes=[
            pltpu.VMEM((slots, sum_keys.shape[0], G * (DK + DV)), jnp.bfloat16),
            pltpu.VMEM((tokens, width), jnp.bfloat16),
            pltpu.VMEM((tokens, H * DV), jnp.bfloat16),
            pltpu.VMEM((rows, PAD), jnp.bfloat16),
            pltpu.VMEM((G, keys, PAD), jnp.bfloat16),
            pltpu.VMEM((G, DV, keys), jnp.bfloat16),
            [pltpu.VMEM((keys, ROWS), jnp.float32)] * (tiles // G),
            pltpu.VMEM((tiles, 8, ROWS), jnp.float32),
            pltpu.VMEM((tiles, 8, ROWS), jnp.float32),
            pltpu.VMEM((tiles, DV, ROWS), jnp.float32),
            dma((3,)),
            dma((G,)),
            dma((ROUNDS * 2,)),
            dma((ROUNDS * 2,)),
            dma((ROUNDS * 3 + 3,)),
            dma((ROUNDS * 3 + 3,)),
            dma((ROUNDS * COLS + 1,)),
            dma((ROUNDS * COLS + 1,)),
            pltpu.SemaphoreType.REGULAR((3,)),
        ],
        compiler_params=pltpu.CompilerParams(collective_id=0, has_side_effects=True, vmem_limit_bytes=VMEM),
        name="fused",
    )(queries, sum_keys, sum_values, limits, valid_tokens)


def solution(mesh):
    depth = mesh.shape["seq"] // (COLS * CORES)
    placed = (
        P(("grp", "seq"), None),
        P(("grp", "seq"), None),
        P(("grp", "seq"), None),
        P("grp"),
        P("grp"),
    )
    return jax.shard_map(
        functools.partial(per_device, depth),
        mesh=mesh,
        in_specs=placed,
        out_specs=P(("grp", "seq"), None),
        check_vma=False,
    )
```

```python
import functools

import jax
import jax.numpy as jnp
from jax import lax
from jax.experimental import pallas as pl
from jax.experimental.pallas import tpu as pltpu
from jax.sharding import PartitionSpec as P

H = 64
G = 4
DK = 192
DV = 128
STRIDE = 16
CBLOCK = 32
QB = 64

CORES = 2
COLS = 4
UP_ROUNDS = 3
ROUNDS = 5
UP, DOWN = 0, 1
PAD = 256
ROWS = 256
AHEAD = 5
VMEM = 61 * 2**20
NEG = -1e30
PARTS = ((1, 2, 3, 4), (5, 6, -1, -2), (7, 8, -3, -4), (-5, -6, 9, 0))
HOMES = (((1, 2), (2, 2), (3, 0)), ((0, 0), (0, 2), (1, 0), (2, 0), (3, 2)))
SCALE = float(DK) ** -0.5 * 1.4426950408889634


def place(depth):
    me = lax.axis_index("seq")
    return me // (depth * CORES), lax.rem(me // CORES, depth), lax.rem(me, CORES)


def spread_queries(q_ref, qp):
    tokens = q_ref.shape[0]
    lane = lax.broadcasted_iota(jnp.int32, (tokens, PAD), 1)
    token = lax.broadcasted_iota(jnp.int32, (tokens, PAD), 0)
    for head in range(H):
        group = head // (H // G)
        low = group % 2 == 0
        first = head * DK
        spare = DK if low else 0
        marks = jnp.where(lane == spare + token // QB, 1.0, 0.0)
        window = q_ref[:, pl.ds(first - first % 128, PAD)].astype(jnp.float32)
        if low != (first % 128 == 0):
            window = pltpu.roll(window, PAD - 64 if low else 64, 1)
        held = jnp.where((lane < DK) if low else (lane >= PAD - DK), window, marks)
        qp[head * tokens : (head + 1) * tokens, :] = held.astype(jnp.bfloat16)


def spread_keys(part, depth, caps, kv, kp, vp):
    col, z, core = place(depth)
    keys = CORES * COLS * 4 * 8
    slots = keys // 8
    block = kv[pl.ds(part * slots, slots)].astype(jnp.float32).reshape(keys, G * (DK + DV))
    at = lax.broadcasted_iota(jnp.int32, (keys, PAD), 0)
    lane = lax.broadcasted_iota(jnp.int32, (keys, PAD), 1)
    spot = (at // 16) % 4
    away = jnp.full(spot.shape, PARTS[part][3])
    for place_ in range(3):
        away = jnp.where(spot == place_, PARTS[part][place_], away)
    source_z = (z + away + depth) % depth
    source = (at // 64) * (depth * CORES) + source_z * CORES + (at // 8) % CORES
    ids = source * 8 + at % 8
    for group in range(G):
        low = group % 2 == 0
        first = group * DK
        spare = DK if low else 0
        hidden = ((lane == spare) & (ids >= caps[0])) | ((lane == spare + 1) & (ids >= caps[1]))
        bias = jnp.where(hidden, NEG, 0.0)
        window = block[:, first - first % 128 : first - first % 128 + PAD]
        held = jnp.where((lane < DK) if low else (lane >= PAD - DK), window, bias)
        kp[group] = held.astype(jnp.bfloat16)
        vp[group] = block[:, G * DK + group * DV : G * DK + (group + 1) * DV].T.astype(jnp.bfloat16)


def fold(last, tokens, qp, kp, vp, buffers, top, total, held, out_ref, leave):
    per_tile = ROWS // tokens
    tiles = H // G // per_tile

    def scores(group, u):
        rows = pl.ds(pl.multiple_of((group * tiles + u) * ROWS, ROWS), ROWS)
        score = lax.dot_general(kp[group], qp[rows, :], (((1,), (1,)), ((), ())), preferred_element_type=jnp.float32)
        buffers[u][...] = score
        return jnp.broadcast_to(jnp.max(score, axis=0, keepdims=True) * SCALE, (8, ROWS))

    def blend(group, u, best):
        tile = group * tiles + u
        old_top = top[tile]
        new_top = jnp.maximum(old_top, best)
        score = buffers[u][...]
        keys = score.shape[0]
        weight = jnp.exp2(score.reshape(keys // 8, 8, ROWS) * SCALE - new_top[None])
        added = jnp.sum(weight, axis=0)
        value = jnp.dot(vp[group], weight.reshape(keys, ROWS).astype(jnp.bfloat16), preferred_element_type=jnp.float32)
        rescale = jnp.exp2(old_top - new_top)
        added = added + total[tile] * rescale
        value = value + (held[tile].reshape(DV // 8, 8, ROWS) * rescale[None]).reshape(DV, ROWS)
        if last:
            done = (value * (1.0 / jnp.sum(added, axis=0, keepdims=True))).T.astype(jnp.bfloat16)
            for b in range(per_tile):
                head = tile * per_tile + b
                out_ref[:, pl.ds(pl.multiple_of(head * DV, DV), DV)] = done[b * tokens : (b + 1) * tokens]
        else:
            top[tile] = new_top
            total[tile] = added
            held[tile] = value

    def step(group, bests):
        for u in range(tiles):
            at = u + AHEAD
            if at < tiles:
                new = scores(group, at)
            else:
                new = scores(jnp.minimum(group + 1, G - 1), at - tiles)
            blend(group, u, bests[0])
            bests = bests[1:] + (new,)
        if last:
            leave(group).start()
        return bests

    lax.fori_loop(0, G, step, tuple(scores(0, u) for u in range(AHEAD)))


def slot_of(part, column, spot):
    return ((part * COLS + column) * 4 + spot) * CORES


def kernel(
    depth, q_any, k_any, v_any, limits, valid, out_any, kv, q_ref, out_ref, qp, kp, vp, buffers, top, total, held,
    own_sem, out_sem, z_send, z_recv, x_send, x_recv, d_send, d_recv, ready,
):
    col, z, core = place(depth)
    way = 1 - 2 * core
    mesh_id = pl.DeviceIdType.MESH

    def device(dx, dz, dc):
        target = lax.rem(col + dx, COLS) * (depth * CORES) + lax.rem(z + dz + depth, depth) * CORES
        return {"seq": target + lax.rem(core + dc, CORES)}

    def column(k):
        return lax.rem(col - k + COLS, COLS)

    def push(src, dst, send, recv, target):
        pltpu.make_async_remote_copy(
            src_ref=src, dst_ref=dst, send_sem=send, recv_sem=recv, device_id=target, device_id_type=mesh_id
        ).start()

    def arrived(slab, sem):
        pltpu.make_async_copy(slab, slab, sem).wait()

    def chip(part, column_, spot):
        return kv.at[pl.ds(slot_of(part, column_, spot), CORES)]

    own = slot_of(3, col, 3) + core
    loads = [
        pltpu.make_async_copy(k_any, kv.at[own, :, 0 : G * DK], own_sem.at[0]),
        pltpu.make_async_copy(v_any, kv.at[own, :, G * DK : G * (DK + DV)], own_sem.at[1]),
        pltpu.make_async_copy(q_any, q_ref, own_sem.at[2]),
    ]
    for c in loads:
        c.start()

    first_chip = (col == 0) & (z == 0)

    def turn(at_z):
        return jnp.where((col == 0) & (core == 0) & (at_z == 0), depth, at_z)

    def along(dz):
        return turn(lax.rem(z + dz + depth, depth))

    barrier = pltpu.get_barrier_semaphore()

    def greet(peer):
        pl.semaphore_signal(barrier, inc=1, device_id=peer, device_id_type=mesh_id)

    for dx in (1, 2, 3):
        pl.when(col >= dx)(lambda: greet(device(COLS - dx, 0, 0)))
    pl.when(col == COLS - 2)(lambda: greet(device(1, 0, 0)))
    pl.when(jnp.logical_not(first_chip) | (core == 1))(lambda: greet(device(0, 0, 1)))
    my_turn = turn(z)
    expected = jnp.where(col == COLS - 1, 1, COLS - 1 - col) + jnp.where(first_chip & (core == 1), 0, 1)
    for dz in (1, 2, -1, -2):
        pl.when(along(dz) > my_turn)(lambda: greet(device(0, dz, 0)))
        expected = expected + jnp.where(along(dz) < my_turn, 1, 0)
    pl.semaphore_wait(barrier, expected)

    def answer(i, peer):
        pl.semaphore_signal(ready.at[i], inc=1, device_id=peer, device_id_type=mesh_id)

    for i in (1, 2):
        pl.when(along(-way * i) < my_turn)(lambda: answer(i - 1, device(0, -way * i, 0)))
    pl.when(first_chip & (core == 0))(lambda: answer(2, device(0, 0, 1)))

    loads[0].wait()
    loads[1].wait()
    mine = kv.at[pl.ds(own, 1)]
    theirs = kv.at[pl.ds(slot_of(3, col, 3) + 1 - core, 1)]

    def share():
        push(mine, mine, d_send.at[ROUNDS * COLS], d_recv.at[ROUNDS * COLS], device(0, 0, 1))
        arrived(theirs, d_recv.at[ROUNDS * COLS])

    def home(direction, r):
        if r >= UP_ROUNDS:
            return HOMES[DOWN][r]
        return tuple(jnp.where(direction == UP, a, b) for a, b in zip(HOMES[UP][r], HOMES[DOWN][r]))

    def from_afar(r, column_, i):
        part, spot = home(core, r)
        return chip(part, column_, spot + i - 1)

    def onward(r, src, i):
        at = from_afar(r, col, i)
        push(src, at, z_send.at[r * 2 + i - 1], z_recv.at[r * 2 + i - 1], device(0, way * i, 0))

    def held_back(i):
        return (core == DOWN) & (z < i)

    def relay_source(r):
        return chip(3, col, 3) if r == 0 else from_afar(r - 1, col, 2)

    def across(r, slab):
        two = (col == 1) | (col == 0) if r == ROUNDS else (col == 1) | ((col == 0) & jnp.logical_not(over))
        for dx, to in ((3, col == 0), (2, two), (1, col < COLS - 1)):

            @pl.when(to)
            def _():
                push(slab, slab, x_send.at[r * 3 + dx - 1], x_recv.at[r * 3 + dx - 1], device(dx, 0, 0))

    over = z >= depth // 2
    last_to_share = first_chip & (core == 1)

    @pl.when(jnp.logical_not(last_to_share))
    def _():
        share()
        for i in (2, 1):

            @pl.when((core == UP) & (along(i) > my_turn))
            def _():
                pl.semaphore_wait(ready.at[i - 1], 1)

            pl.when(jnp.logical_not(held_back(i)))(lambda: onward(0, relay_source(0), i))

        across(ROUNDS, chip(3, col, 3))

    def from_across(r, k, slab):
        arrived(slab, x_recv.at[r * 3 + k - 1])
        if k == 3 and r < ROUNDS:

            @pl.when(over)
            def _():
                push(slab, slab, x_send.at[r * 3 + 2], x_recv.at[r * 3 + 1], device(3, 0, 0))

    def slab_of(direction, r, column_):
        part, spot = home(direction, r)
        return kv.at[pl.ds(slot_of(part, column_, spot), CORES if r == ROUNDS - 1 else 2 * CORES)]

    paired = (core == UP) | (z > 0)

    def both(r):
        return (1,) if r == ROUNDS - 1 else (1, 2)

    def chain(r):
        for i in both(r):
            arrived(from_afar(r, col, i), z_recv.at[r * 2 + i - 1])
        for i in reversed(both(r + 1)) if r < ROUNDS - 1 else ():
            further = jnp.logical_not(held_back(i))
            if r >= UP_ROUNDS - 1:
                further = further & (core == DOWN)
            pl.when(further)(lambda: onward(r + 1, relay_source(r + 1), i))
        slab = slab_of(core, r, col)
        across(r, slab)

        @pl.when(paired)
        def _():
            push(slab, slab, d_send.at[r * COLS], d_recv.at[r * COLS], device(0, 0, 1))

    def pass_on(r):
        for k in (3, 1, 2):

            @pl.when(k <= col)
            def _():
                slab = slab_of(core, r, column(k))
                from_across(r, k, slab)
                push(slab, slab, d_send.at[r * COLS + k], d_recv.at[r * COLS + k], device(0, 0, 1))

    def from_partner(*rounds):
        for r in rounds:
            for k in range(COLS):

                @pl.when((k <= col) & ((core == DOWN) | (z > 0)) if k == 0 else k <= col)
                def _():
                    arrived(slab_of(1 - core, r, column(k)), d_recv.at[r * COLS + k])

    tokens = q_ref.shape[0]
    usable = jnp.maximum(lax.shift_right_arithmetic(valid[0] - CBLOCK, 4) + 1, 1)
    first_block = lax.axis_index("seq") * (tokens // QB)
    caps = [jnp.minimum(limits[first_block + b], usable) for b in range(tokens // QB)]

    def weigh(part, last=False):
        spread_keys(part, depth, caps, kv, kp, vp)
        fold(last, tokens, qp, kp, vp, buffers, top, total, held, out_ref, leave)

    def leave(group):
        heads = pl.ds(pl.multiple_of(group * (H // G * DV), 128), H // G * DV)
        return pltpu.make_async_copy(out_ref.at[:, heads], out_any.at[:, heads], out_sem.at[group])

    def prep():
        loads[2].wait()
        spread_queries(q_ref, qp)
        top[...] = jnp.full(top.shape, -1e38, jnp.float32)
        total[...] = jnp.zeros(total.shape, jnp.float32)
        held[...] = jnp.zeros(held.shape, jnp.float32)
        for column_ in range(1, COLS):

            @pl.when(column_ > col)
            def _():
                for part in range(4):
                    unused = kv.at[pl.ds(slot_of(part, column_, 0), 4 * CORES)]
                    unused[...] = jnp.zeros(unused.shape, unused.dtype)

        @pl.when((core == UP) & (z == 0))
        def _():
            for part, spot, spots in ((0, 0, 4), (1, 0, 2), (2, 0, 2), (3, 2, 1)):
                unused = kv.at[pl.ds(slot_of(part, col, spot), spots * CORES)]
                unused[...] = jnp.zeros(unused.shape, unused.dtype)

    up, down = core == UP, core == DOWN
    early = jnp.where(up, jnp.where(first_chip, UP_ROUNDS, jnp.minimum(z // 2, UP_ROUNDS)), 0)
    high_up = up & (early == UP_ROUNDS)
    sees_more = jnp.logical_not(first_chip)
    near_late = up & (early < 2)

    for r in range(UP_ROUNDS):
        pl.when(r < early)(lambda: chain(r))
    pl.when(early >= 2)(lambda: pass_on(0))
    pl.when(high_up)(lambda: pass_on(1))
    prep()

    @pl.when(up)
    def _():
        pl.when(high_up)(lambda: pass_on(2))
        from_partner(0, 1)

    @pl.when(down)
    def _():
        chain(0)
        chain(1)
        pass_on(0)
        pass_on(1)
        chain(2)

        @pl.when(last_to_share)
        def _():
            pl.semaphore_wait(ready.at[2], 1)
            share()
            across(ROUNDS, chip(3, col, 3))

        for i in (1, 2):

            @pl.when(held_back(i))
            def _():
                pl.semaphore_wait(ready.at[i - 1], 1)
                for r in range(ROUNDS - 1):
                    onward(r, relay_source(r), i)

    pl.when(sees_more)(lambda: weigh(0))

    @pl.when(up)
    def _():
        @pl.when(near_late)
        def _():
            pl.when(early < 1)(lambda: chain(0))
            chain(1)
            pass_on(0)

        from_partner(2)

    @pl.when(down)
    def _():
        chain(3)
        pl.when(held_back(1))(lambda: onward(4, relay_source(4), 1))
        pass_on(2)
        pl.when(jnp.logical_not(over))(lambda: chain(4))
        from_partner(0)

    pl.when(sees_more)(lambda: weigh(1))

    @pl.when(up)
    def _():
        pl.when(early < UP_ROUNDS)(lambda: chain(2))
        pl.when(jnp.logical_not(high_up))(lambda: pass_on(1))
        from_partner(3)

    @pl.when(down)
    def _():
        pass_on(3)
        pl.when(over)(lambda: chain(4))
        pl.when(jnp.logical_not(over))(lambda: pass_on(4))
        from_partner(1)

    pl.when(sees_more)(lambda: weigh(2))

    @pl.when(up)
    def _():
        pl.when(jnp.logical_not(high_up))(lambda: pass_on(2))
        from_partner(4)

    @pl.when(down)
    def _():
        pl.when(over)(lambda: pass_on(4))
        from_partner(2)

    for k in (3, 1, 2):
        pl.when(k <= col)(lambda: from_across(ROUNDS, k, chip(3, column(k), 3)))
    weigh(3, True)
    for group in range(G):
        leave(group).wait()

    def across_left(r, slab):
        two = (col == 1) | (col == 0) if r == ROUNDS else (col == 1) | ((col == 0) & jnp.logical_not(over))
        three = (col == 0) if r == ROUNDS else (col == 0) | ((col == COLS - 1) & over)
        for dx, to in ((1, col < COLS - 1), (2, two), (3, three)):
            pl.when(to)(lambda: arrived(slab, x_send.at[r * 3 + dx - 1]))

    for r in range(ROUNDS):

        @pl.when(down | (r < UP_ROUNDS))
        def _():
            for i in both(r):
                arrived(chip(0, 0, 0), z_send.at[r * 2 + i - 1])
            slab = slab_of(core, r, 0)
            across_left(r, slab)
            for k in range(COLS):
                pl.when((k <= col) & paired if k == 0 else k <= col)(lambda: arrived(slab, d_send.at[r * COLS + k]))

    across_left(ROUNDS, chip(0, 0, 0))
    arrived(mine, d_send.at[ROUNDS * COLS])


def per_device(depth, queries, sum_keys, sum_values, limits, valid_tokens):
    tokens, width = queries.shape
    smem = pl.BlockSpec(memory_space=pltpu.SMEM)
    anywhere = pl.BlockSpec(memory_space=pl.ANY)
    main = pl.BlockSpec(memory_space=pltpu.HBM)
    dma = pltpu.SemaphoreType.DMA
    keys = CORES * COLS * 4 * sum_keys.shape[0]
    rows = H * tokens
    tiles = rows // ROWS
    slots = 4 * CORES * COLS * 4
    return pl.pallas_call(
        functools.partial(kernel, depth),
        out_shape=pltpu.VMEM((tokens, H * DV), jnp.bfloat16),
        in_specs=[main, main, main, smem, smem],
        out_specs=anywhere,
        scratch_shapes=[
            pltpu.VMEM((slots, sum_keys.shape[0], G * (DK + DV)), jnp.bfloat16),
            pltpu.VMEM((tokens, width), jnp.bfloat16),
            pltpu.VMEM((tokens, H * DV), jnp.bfloat16),
            pltpu.VMEM((rows, PAD), jnp.bfloat16),
            pltpu.VMEM((G, keys, PAD), jnp.bfloat16),
            pltpu.VMEM((G, DV, keys), jnp.bfloat16),
            [pltpu.VMEM((keys, ROWS), jnp.float32)] * (tiles // G),
            pltpu.VMEM((tiles, 8, ROWS), jnp.float32),
            pltpu.VMEM((tiles, 8, ROWS), jnp.float32),
            pltpu.VMEM((tiles, DV, ROWS), jnp.float32),
            dma((3,)),
            dma((G,)),
            dma((ROUNDS * 2,)),
            dma((ROUNDS * 2,)),
            dma((ROUNDS * 3 + 3,)),
            dma((ROUNDS * 3 + 3,)),
            dma((ROUNDS * COLS + 1,)),
            dma((ROUNDS * COLS + 1,)),
            pltpu.SemaphoreType.REGULAR((3,)),
        ],
        compiler_params=pltpu.CompilerParams(collective_id=0, has_side_effects=True, vmem_limit_bytes=VMEM),
        name="fused",
    )(queries, sum_keys, sum_values, limits, valid_tokens)


def solution(mesh):
    depth = mesh.shape["seq"] // (COLS * CORES)
    placed = (
        P(("grp", "seq"), None),
        P(("grp", "seq"), None),
        P(("grp", "seq"), None),
        P("grp"),
        P("grp"),
    )
    return jax.shard_map(
        functools.partial(per_device, depth),
        mesh=mesh,
        in_specs=placed,
        out_specs=P(("grp", "seq"), None),
        check_vma=False,
    )
```

```python
import functools

import jax
import jax.numpy as jnp
from jax import lax
from jax.experimental import pallas as pl
from jax.experimental.pallas import tpu as pltpu
from jax.sharding import PartitionSpec as P

H = 64
G = 4
DK = 192
DV = 128
STRIDE = 16
CBLOCK = 32
QB = 64

CORES = 2
COLS = 4
UP_ROUNDS = 3
ROUNDS = 5
UP, DOWN = 0, 1
PAD = 256
ROWS = 256
AHEAD = 5
VMEM = 61 * 2**20
NEG = -1e30
PARTS = ((1, 2, 3, 4), (5, 6, -1, -2), (7, 8, -3, -4), (-5, -6, 9, 0))
HOMES = (((1, 2), (2, 2), (3, 0)), ((0, 0), (0, 2), (1, 0), (2, 0), (3, 2)))
SCALE = float(DK) ** -0.5 * 1.4426950408889634


def place(depth):
    me = lax.axis_index("seq")
    return me // (depth * CORES), lax.rem(me // CORES, depth), lax.rem(me, CORES)


def spread_queries(q_ref, qp):
    tokens = q_ref.shape[0]
    lane = lax.broadcasted_iota(jnp.int32, (tokens, PAD), 1)
    token = lax.broadcasted_iota(jnp.int32, (tokens, PAD), 0)
    for head in range(H):
        group = head // (H // G)
        low = group % 2 == 0
        first = head * DK
        spare = DK if low else 0
        marks = jnp.where(lane == spare + token // QB, 1.0, 0.0)
        window = q_ref[:, pl.ds(first - first % 128, PAD)].astype(jnp.float32)
        if low != (first % 128 == 0):
            window = pltpu.roll(window, PAD - 64 if low else 64, 1)
        held = jnp.where((lane < DK) if low else (lane >= PAD - DK), window, marks)
        qp[head * tokens : (head + 1) * tokens, :] = held.astype(jnp.bfloat16)


def spread_keys(part, depth, caps, kv, kp, vp):
    col, z, core = place(depth)
    keys = CORES * COLS * 4 * 8
    slots = keys // 8
    block = kv[pl.ds(part * slots, slots)].astype(jnp.float32).reshape(keys, G * (DK + DV))
    at = lax.broadcasted_iota(jnp.int32, (keys, PAD), 0)
    lane = lax.broadcasted_iota(jnp.int32, (keys, PAD), 1)
    spot = (at // 16) % 4
    away = jnp.full(spot.shape, PARTS[part][3])
    for place_ in range(3):
        away = jnp.where(spot == place_, PARTS[part][place_], away)
    source_z = (z + away + depth) % depth
    source = (at // 64) * (depth * CORES) + source_z * CORES + (at // 8) % CORES
    ids = source * 8 + at % 8
    for group in range(G):
        low = group % 2 == 0
        first = group * DK
        spare = DK if low else 0
        hidden = ((lane == spare) & (ids >= caps[0])) | ((lane == spare + 1) & (ids >= caps[1]))
        bias = jnp.where(hidden, NEG, 0.0)
        window = block[:, first - first % 128 : first - first % 128 + PAD]
        held = jnp.where((lane < DK) if low else (lane >= PAD - DK), window, bias)
        kp[group] = held.astype(jnp.bfloat16)
        vp[group] = block[:, G * DK + group * DV : G * DK + (group + 1) * DV].T.astype(jnp.bfloat16)


def fold(last, tokens, qp, kp, vp, buffers, top, total, held, out_ref, leave):
    per_tile = ROWS // tokens
    tiles = H // G // per_tile

    def scores(group, u):
        rows = pl.ds(pl.multiple_of((group * tiles + u) * ROWS, ROWS), ROWS)
        score = lax.dot_general(kp[group], qp[rows, :], (((1,), (1,)), ((), ())), preferred_element_type=jnp.float32)
        buffers[u][...] = score
        return jnp.broadcast_to(jnp.max(score, axis=0, keepdims=True) * SCALE, (8, ROWS))

    def mix(group, u, best):
        tile = group * tiles + u
        old_top = top[tile]
        new_top = jnp.maximum(old_top, best)
        score = buffers[u][...]
        keys = score.shape[0]
        weight = jnp.exp2(score.reshape(keys // 8, 8, ROWS) * SCALE - new_top[None])
        rescale = jnp.exp2(old_top - new_top)
        added = jnp.sum(weight, axis=0) + total[tile] * rescale
        value = jnp.dot(vp[group], weight.reshape(keys, ROWS).astype(jnp.bfloat16), preferred_element_type=jnp.float32)
        return new_top, rescale, added, value

    def add(group, u, mixed):
        tile = group * tiles + u
        new_top, rescale, added, value = mixed
        value = value + (held[tile].reshape(DV // 8, 8, ROWS) * rescale[None]).reshape(DV, ROWS)
        if last:
            done = (value * (1.0 / jnp.sum(added, axis=0, keepdims=True))).T.astype(jnp.bfloat16)
            for b in range(per_tile):
                head = tile * per_tile + b
                out_ref[:, pl.ds(pl.multiple_of(head * DV, DV), DV)] = done[b * tokens : (b + 1) * tokens]
        else:
            top[tile] = new_top
            total[tile] = added
            held[tile] = value

    def step(group, bests):
        waiting = None
        for u in range(tiles):
            at = u + AHEAD
            if at < tiles:
                new = scores(group, at)
            else:
                new = scores(jnp.minimum(group + 1, G - 1), at - tiles)
            mixed = mix(group, u, bests[0])
            if waiting is not None:
                add(group, u - 1, waiting)
            waiting = mixed
            bests = bests[1:] + (new,)
        add(group, tiles - 1, waiting)
        if last:
            leave(group).start()
        return bests

    lax.fori_loop(0, G, step, tuple(scores(0, u) for u in range(AHEAD)))


def slot_of(part, column, spot):
    return ((part * COLS + column) * 4 + spot) * CORES


def kernel(
    depth, q_any, k_any, v_any, limits, valid, out_any, kv, q_ref, out_ref, qp, kp, vp, buffers, top, total, held,
    own_sem, out_sem, z_send, z_recv, x_send, x_recv, d_send, d_recv, ready,
):
    col, z, core = place(depth)
    way = 1 - 2 * core
    mesh_id = pl.DeviceIdType.MESH

    def device(dx, dz, dc):
        target = lax.rem(col + dx, COLS) * (depth * CORES) + lax.rem(z + dz + depth, depth) * CORES
        return {"seq": target + lax.rem(core + dc, CORES)}

    def column(k):
        return lax.rem(col - k + COLS, COLS)

    def push(src, dst, send, recv, target):
        pltpu.make_async_remote_copy(
            src_ref=src, dst_ref=dst, send_sem=send, recv_sem=recv, device_id=target, device_id_type=mesh_id
        ).start()

    def arrived(slab, sem):
        pltpu.make_async_copy(slab, slab, sem).wait()

    def chip(part, column_, spot):
        return kv.at[pl.ds(slot_of(part, column_, spot), CORES)]

    own = slot_of(3, col, 3) + core
    loads = [
        pltpu.make_async_copy(k_any, kv.at[own, :, 0 : G * DK], own_sem.at[0]),
        pltpu.make_async_copy(v_any, kv.at[own, :, G * DK : G * (DK + DV)], own_sem.at[1]),
        pltpu.make_async_copy(q_any, q_ref, own_sem.at[2]),
    ]
    for c in loads:
        c.start()

    first_chip = (col == 0) & (z == 0)

    def turn(at_z):
        return jnp.where((col == 0) & (core == 0) & (at_z == 0), depth, at_z)

    def along(dz):
        return turn(lax.rem(z + dz + depth, depth))

    barrier = pltpu.get_barrier_semaphore()

    def greet(peer):
        pl.semaphore_signal(barrier, inc=1, device_id=peer, device_id_type=mesh_id)

    for dx in (1, 2, 3):
        pl.when(col >= dx)(lambda: greet(device(COLS - dx, 0, 0)))
    pl.when(col == COLS - 2)(lambda: greet(device(1, 0, 0)))
    pl.when(jnp.logical_not(first_chip) | (core == 1))(lambda: greet(device(0, 0, 1)))
    my_turn = turn(z)
    expected = jnp.where(col == COLS - 1, 1, COLS - 1 - col) + jnp.where(first_chip & (core == 1), 0, 1)
    for dz in (1, 2, -1, -2):
        pl.when(along(dz) > my_turn)(lambda: greet(device(0, dz, 0)))
        expected = expected + jnp.where(along(dz) < my_turn, 1, 0)
    pl.semaphore_wait(barrier, expected)

    def answer(i, peer):
        pl.semaphore_signal(ready.at[i], inc=1, device_id=peer, device_id_type=mesh_id)

    for i in (1, 2):
        pl.when(along(-way * i) < my_turn)(lambda: answer(i - 1, device(0, -way * i, 0)))
    pl.when(first_chip & (core == 0))(lambda: answer(2, device(0, 0, 1)))

    loads[0].wait()
    loads[1].wait()
    mine = kv.at[pl.ds(own, 1)]
    theirs = kv.at[pl.ds(slot_of(3, col, 3) + 1 - core, 1)]

    def share():
        push(mine, mine, d_send.at[ROUNDS * COLS], d_recv.at[ROUNDS * COLS], device(0, 0, 1))
        arrived(theirs, d_recv.at[ROUNDS * COLS])

    def home(direction, r):
        if r >= UP_ROUNDS:
            return HOMES[DOWN][r]
        return tuple(jnp.where(direction == UP, a, b) for a, b in zip(HOMES[UP][r], HOMES[DOWN][r]))

    def from_afar(r, column_, i):
        part, spot = home(core, r)
        return chip(part, column_, spot + i - 1)

    def onward(r, src, i):
        at = from_afar(r, col, i)
        push(src, at, z_send.at[r * 2 + i - 1], z_recv.at[r * 2 + i - 1], device(0, way * i, 0))

    def held_back(i):
        return (core == DOWN) & (z < i)

    def relay_source(r):
        return chip(3, col, 3) if r == 0 else from_afar(r - 1, col, 2)

    def across(r, slab):
        two = (col == 1) | (col == 0) if r == ROUNDS else (col == 1) | ((col == 0) & jnp.logical_not(over))
        for dx, to in ((3, col == 0), (2, two), (1, col < COLS - 1)):

            @pl.when(to)
            def _():
                push(slab, slab, x_send.at[r * 3 + dx - 1], x_recv.at[r * 3 + dx - 1], device(dx, 0, 0))

    over = z >= depth // 2
    last_to_share = first_chip & (core == 1)

    @pl.when(jnp.logical_not(last_to_share))
    def _():
        share()
        for i in (2, 1):

            @pl.when((core == UP) & (along(i) > my_turn))
            def _():
                pl.semaphore_wait(ready.at[i - 1], 1)

            pl.when(jnp.logical_not(held_back(i)))(lambda: onward(0, relay_source(0), i))

        across(ROUNDS, chip(3, col, 3))

    def from_across(r, k, slab):
        arrived(slab, x_recv.at[r * 3 + k - 1])
        if k == 3 and r < ROUNDS:

            @pl.when(over)
            def _():
                push(slab, slab, x_send.at[r * 3 + 2], x_recv.at[r * 3 + 1], device(3, 0, 0))

    def slab_of(direction, r, column_):
        part, spot = home(direction, r)
        return kv.at[pl.ds(slot_of(part, column_, spot), CORES if r == ROUNDS - 1 else 2 * CORES)]

    paired = (core == UP) | (z > 0)

    def both(r):
        return (1,) if r == ROUNDS - 1 else (1, 2)

    def chain(r):
        arrived(from_afar(r, col, both(r)[-1]), z_recv.at[r * 2 + both(r)[-1] - 1])
        for i in reversed(both(r + 1)) if r < ROUNDS - 1 else ():
            further = jnp.logical_not(held_back(i))
            if r >= UP_ROUNDS - 1:
                further = further & (core == DOWN)
            pl.when(further)(lambda: onward(r + 1, relay_source(r + 1), i))
        if r < ROUNDS - 1:
            arrived(from_afar(r, col, 1), z_recv.at[r * 2])
        slab = slab_of(core, r, col)
        across(r, slab)

        @pl.when(paired)
        def _():
            push(slab, slab, d_send.at[r * COLS], d_recv.at[r * COLS], device(0, 0, 1))

    def pass_on(r):
        for k in (3, 1, 2):

            @pl.when(k <= col)
            def _():
                slab = slab_of(core, r, column(k))
                from_across(r, k, slab)
                push(slab, slab, d_send.at[r * COLS + k], d_recv.at[r * COLS + k], device(0, 0, 1))

    def from_partner(*rounds):
        for r in rounds:
            for k in range(COLS):

                @pl.when((k <= col) & ((core == DOWN) | (z > 0)) if k == 0 else k <= col)
                def _():
                    arrived(slab_of(1 - core, r, column(k)), d_recv.at[r * COLS + k])

    tokens = q_ref.shape[0]
    usable = jnp.maximum(lax.shift_right_arithmetic(valid[0] - CBLOCK, 4) + 1, 1)
    first_block = lax.axis_index("seq") * (tokens // QB)
    caps = [jnp.minimum(limits[first_block + b], usable) for b in range(tokens // QB)]

    def weigh(part, last=False):
        spread_keys(part, depth, caps, kv, kp, vp)
        fold(last, tokens, qp, kp, vp, buffers, top, total, held, out_ref, leave)

    def leave(group):
        heads = pl.ds(pl.multiple_of(group * (H // G * DV), 128), H // G * DV)
        return pltpu.make_async_copy(out_ref.at[:, heads], out_any.at[:, heads], out_sem.at[group])

    def prep():
        loads[2].wait()
        spread_queries(q_ref, qp)
        top[...] = jnp.full(top.shape, -1e38, jnp.float32)
        total[...] = jnp.zeros(total.shape, jnp.float32)
        held[...] = jnp.zeros(held.shape, jnp.float32)
        for column_ in range(1, COLS):

            @pl.when(column_ > col)
            def _():
                for part in range(4):
                    unused = kv.at[pl.ds(slot_of(part, column_, 0), 4 * CORES)]
                    unused[...] = jnp.zeros(unused.shape, unused.dtype)

        @pl.when((core == UP) & (z == 0))
        def _():
            for part, spot, spots in ((0, 0, 4), (1, 0, 2), (2, 0, 2), (3, 2, 1)):
                unused = kv.at[pl.ds(slot_of(part, col, spot), spots * CORES)]
                unused[...] = jnp.zeros(unused.shape, unused.dtype)

    up, down = core == UP, core == DOWN
    early = jnp.where(up, jnp.where(first_chip, UP_ROUNDS, jnp.minimum(z // 2, UP_ROUNDS)), 0)
    high_up = up & (early == UP_ROUNDS)
    sees_more = jnp.logical_not(first_chip)
    near_late = up & (early < 2)

    for r in range(UP_ROUNDS):
        pl.when(r < early)(lambda: chain(r))
    pl.when(early >= 2)(lambda: pass_on(0))
    pl.when(high_up)(lambda: pass_on(1))
    prep()

    @pl.when(up)
    def _():
        pl.when(high_up)(lambda: pass_on(2))
        from_partner(0, 1)

    @pl.when(down)
    def _():
        chain(0)
        chain(1)
        pass_on(0)
        pass_on(1)
        chain(2)

        @pl.when(last_to_share)
        def _():
            pl.semaphore_wait(ready.at[2], 1)
            share()
            across(ROUNDS, chip(3, col, 3))

        for i in (1, 2):

            @pl.when(held_back(i))
            def _():
                pl.semaphore_wait(ready.at[i - 1], 1)
                for r in range(ROUNDS - 1):
                    onward(r, relay_source(r), i)

    pl.when(sees_more)(lambda: weigh(0))

    @pl.when(up)
    def _():
        @pl.when(near_late)
        def _():
            pl.when(early < 1)(lambda: chain(0))
            chain(1)
            pass_on(0)

        from_partner(2)

    @pl.when(down)
    def _():
        chain(3)
        pl.when(held_back(1))(lambda: onward(4, relay_source(4), 1))
        pass_on(2)
        pl.when(jnp.logical_not(over))(lambda: chain(4))
        from_partner(0)

    pl.when(sees_more)(lambda: weigh(1))

    @pl.when(up)
    def _():
        pl.when(early < UP_ROUNDS)(lambda: chain(2))
        pl.when(jnp.logical_not(high_up))(lambda: pass_on(1))
        from_partner(3)

    @pl.when(down)
    def _():
        pass_on(3)
        pl.when(over)(lambda: chain(4))
        pl.when(jnp.logical_not(over))(lambda: pass_on(4))
        from_partner(1)

    pl.when(sees_more)(lambda: weigh(2))

    @pl.when(up)
    def _():
        pl.when(jnp.logical_not(high_up))(lambda: pass_on(2))
        from_partner(4)

    @pl.when(down)
    def _():
        pl.when(over)(lambda: pass_on(4))
        from_partner(2)

    for k in (3, 1, 2):
        pl.when(k <= col)(lambda: from_across(ROUNDS, k, chip(3, column(k), 3)))
    weigh(3, True)
    for group in range(G):
        leave(group).wait()

    def across_left(r, slab):
        two = (col == 1) | (col == 0) if r == ROUNDS else (col == 1) | ((col == 0) & jnp.logical_not(over))
        three = (col == 0) if r == ROUNDS else (col == 0) | ((col == COLS - 1) & over)
        for dx, to in ((1, col < COLS - 1), (2, two), (3, three)):
            pl.when(to)(lambda: arrived(slab, x_send.at[r * 3 + dx - 1]))

    for r in range(ROUNDS):

        @pl.when(down | (r < UP_ROUNDS))
        def _():
            for i in both(r):
                arrived(chip(0, 0, 0), z_send.at[r * 2 + i - 1])
            slab = slab_of(core, r, 0)
            across_left(r, slab)
            for k in range(COLS):
                pl.when((k <= col) & paired if k == 0 else k <= col)(lambda: arrived(slab, d_send.at[r * COLS + k]))

    across_left(ROUNDS, chip(0, 0, 0))
    arrived(mine, d_send.at[ROUNDS * COLS])


def per_device(depth, queries, sum_keys, sum_values, limits, valid_tokens):
    tokens, width = queries.shape
    smem = pl.BlockSpec(memory_space=pltpu.SMEM)
    anywhere = pl.BlockSpec(memory_space=pl.ANY)
    main = pl.BlockSpec(memory_space=pltpu.HBM)
    dma = pltpu.SemaphoreType.DMA
    keys = CORES * COLS * 4 * sum_keys.shape[0]
    rows = H * tokens
    tiles = rows // ROWS
    slots = 4 * CORES * COLS * 4
    return pl.pallas_call(
        functools.partial(kernel, depth),
        out_shape=pltpu.VMEM((tokens, H * DV), jnp.bfloat16),
        in_specs=[main, main, main, smem, smem],
        out_specs=anywhere,
        scratch_shapes=[
            pltpu.VMEM((slots, sum_keys.shape[0], G * (DK + DV)), jnp.bfloat16),
            pltpu.VMEM((tokens, width), jnp.bfloat16),
            pltpu.VMEM((tokens, H * DV), jnp.bfloat16),
            pltpu.VMEM((rows, PAD), jnp.bfloat16),
            pltpu.VMEM((G, keys, PAD), jnp.bfloat16),
            pltpu.VMEM((G, DV, keys), jnp.bfloat16),
            [pltpu.VMEM((keys, ROWS), jnp.float32)] * (tiles // G),
            pltpu.VMEM((tiles, 8, ROWS), jnp.float32),
            pltpu.VMEM((tiles, 8, ROWS), jnp.float32),
            pltpu.VMEM((tiles, DV, ROWS), jnp.float32),
            dma((3,)),
            dma((G,)),
            dma((ROUNDS * 2,)),
            dma((ROUNDS * 2,)),
            dma((ROUNDS * 3 + 3,)),
            dma((ROUNDS * 3 + 3,)),
            dma((ROUNDS * COLS + 1,)),
            dma((ROUNDS * COLS + 1,)),
            pltpu.SemaphoreType.REGULAR((3,)),
        ],
        compiler_params=pltpu.CompilerParams(collective_id=0, has_side_effects=True, vmem_limit_bytes=VMEM),
        name="fused",
    )(queries, sum_keys, sum_values, limits, valid_tokens)


def solution(mesh):
    depth = mesh.shape["seq"] // (COLS * CORES)
    placed = (
        P(("grp", "seq"), None),
        P(("grp", "seq"), None),
        P(("grp", "seq"), None),
        P("grp"),
        P("grp"),
    )
    return jax.shard_map(
        functools.partial(per_device, depth),
        mesh=mesh,
        in_specs=placed,
        out_specs=P(("grp", "seq"), None),
        check_vma=False,
    )
```
